256 devices in a mesh: ex: 8 (over z), ctx: 32 (over x, y, core).
Axes of the slice: x: 4, y: 4, z: 8, core: 2. Of those that a mesh axis runs over, the one named last changes fastest.
Arguments:
- stream: bfloat16 [8, 256, 32768], P('ex', None, 'ctx'), may hold values from -6 to 6
- cotangent: bfloat16 [8, 256, 32768], P('ex', None, 'ctx'), may hold values from -6 to 6
- base_ids: int32 [8, 32768], P('ex', 'ctx'), may hold values from 0 to 4
- clip_bound: int32 [8], P('ex'), may hold values from 1 to 4
- w_value: bfloat16 [256, 256], replicated, may hold values from -2 to 2
- w_gate: bfloat16 [256, 256], replicated, may hold values from -0.375 to 0.375
- filter_taps: float32 [256, 32768], P('ctx', 'ex'), may hold values from -0.03125 to 0.03125
- filter_bias: float32 [256], P('ctx'), may hold values from 0.1 to 1.9
Outputs:
- input_grad: bfloat16 [8, 256, 32768], P('ex', None, 'ctx')
- filter_grad: float32 [256, 32768], P('ctx', 'ex')
The draws below stay inside these ranges and needn't reach their ends.
All inputs are finite; a program needn't handle non-finite values.
Results may differ from the reference program's by a relative error of at most 0.015.
Values may be sent and summed in bfloat16 or wider, within the bound.
No kernel may reach another device: no remote copies, remote signals or barrier semaphores. Data moves between devices by JAX's collectives and lax.ppermute only.
A program may use at most 128 MiB of HBM per device.

```python
import jax
import jax.numpy as jnp
from jax import lax

D = 256
TOK_DEV = 1024
LENGTH = 32768
EXAMPLES = 8
N_CTX = 32


def draw_w_value(key, part):
    key_entries = jax.random.fold_in(key, 11)
    key_jitter = jax.random.fold_in(key, 12)
    rising = 0.3 * 10.0 ** (jnp.arange(D, dtype=jnp.float32) / D)
    jitter = jnp.exp(jax.random.uniform(key_jitter, (D,), jnp.float32, -0.35, 0.35))
    row_scale = rising * jitter
    entries = jax.random.normal(key_entries, (D, D), jnp.float32)
    return (row_scale[:, None] * entries / jnp.sqrt(jnp.float32(D))).astype(jnp.bfloat16)


def with_ends(values, own_key, low, high):
    index_at = [jax.random.randint(jax.random.fold_in(own_key, axis), (), 0, length) for axis, length in enumerate(values.shape)]
    longest = values.shape.index(max(values.shape))
    next_to = index_at[:longest] + [(index_at[longest] + 1) % values.shape[longest]] + index_at[longest + 1:]
    return values.at[tuple(index_at)].set(low).at[tuple(next_to)].set(high)


def block_scale(key, dims, shards, low, high):
    level, own = 1.0, jax.random.fold_in(key, 6)
    for dim, blocks in shards:
        draws = jnp.exp(jax.random.uniform(jax.random.fold_in(own, dim), (blocks,), jnp.float32, low / len(shards), high / len(shards)))
        level = level * jnp.repeat(draws, dims[dim] // blocks).reshape([-1 if axis == dim else 1 for axis in range(len(dims))])
    return level


def noise(stream_key, shape, scale, most, cuts=(), held_as=jnp.bfloat16):
    factor_of = block_scale(stream_key, shape, cuts, -0.22, 0.18) if cuts else 1.0
    values = jax.random.normal(stream_key, shape, jnp.float32) * scale * factor_of
    return jnp.minimum(jnp.maximum(values, -most), most).astype(held_as)


def setup_inputs(seed: int = 0) -> dict:
    seeds = jax.random.split(jax.random.key(seed), 9)
    stream = noise(seeds[0], (EXAMPLES, D, LENGTH), 1.0, 6.0, ((0, 8), (2, 32)))
    cotangent = noise(seeds[1], (EXAMPLES, D, LENGTH), 1.0, 6.0, ((0, 8), (2, 32)))
    base_ids = with_ends(jax.random.randint(seeds[2], (EXAMPLES, LENGTH), 0, 5), jax.random.fold_in(seeds[2], 1), 0, 4).astype(jnp.int32)
    clip_bound = with_ends(jax.random.randint(seeds[3], (EXAMPLES,), 1, 5), jax.random.fold_in(seeds[3], 1), 1, 4).astype(jnp.int32)
    w_value = draw_w_value(jax.random.fold_in(seeds[8], 71), 0)
    w_gate = noise(seeds[5], (D, D), D ** -0.5, 0.375)
    filter_taps = noise(seeds[6], (D, LENGTH), (TOK_DEV * N_CTX) ** -0.5, 0.03125, ((0, 32), (1, 8)), jnp.float32)
    filter_bias = jnp.clip(1.0 + 0.18 * jax.random.normal(seeds[7], (D,), jnp.float32), 0.1, 1.9)
    return {"stream": stream, "cotangent": cotangent, "base_ids": base_ids, "clip_bound": clip_bound, "w_value": w_value, "w_gate": w_gate, "filter_taps": filter_taps, "filter_bias": filter_bias}


unknown_base = 4

def reference(stream, cotangent, base_ids, clip_bound, w_value, w_gate, filter_taps, filter_bias):
    seq_len = stream.shape[2]
    fft_len = 2 * seq_len
    taps_spec = jnp.fft.rfft(filter_taps, n=fft_len, axis=1)
    bias_col = filter_bias[:, None]

    def one_example(running, items):
        tokens_in, cot_raw, ids_row, bound_raw = items
        value = jnp.dot(w_value, tokens_in, preferred_element_type=jnp.float32).astype(jnp.bfloat16)
        gate = jnp.dot(w_gate, tokens_in, preferred_element_type=jnp.float32).astype(jnp.bfloat16)
        keep_mask = (ids_row != unknown_base).astype(jnp.float32)
        masked_cot = (cot_raw.astype(jnp.float32) * keep_mask[None, :]).astype(jnp.bfloat16)
        signal_grad = (gate.astype(jnp.float32) * masked_cot.astype(jnp.float32)).astype(jnp.bfloat16)
        value_wide = value.astype(jnp.float32)
        signal_wide = signal_grad.astype(jnp.float32)
        value_spec = jnp.fft.rfft(value_wide, n=fft_len, axis=1)
        signal_spec = jnp.fft.rfft(signal_wide, n=fft_len, axis=1)
        conv_out = jnp.fft.irfft(taps_spec * value_spec, n=fft_len, axis=1)[:, :seq_len]
        conv_state = (conv_out + bias_col * value_wide).astype(jnp.bfloat16)
        back_out = jnp.fft.irfft(jnp.conj(taps_spec) * signal_spec, n=fft_len, axis=1)[:, :seq_len]
        value_grad = (back_out + bias_col * signal_wide).astype(jnp.bfloat16)
        gate_grad = (conv_state.astype(jnp.float32) * masked_cot.astype(jnp.float32)).astype(jnp.bfloat16)
        input_grad = jnp.dot(w_value.T, value_grad, preferred_element_type=jnp.float32)
        input_grad = input_grad + jnp.dot(w_gate.T, gate_grad, preferred_element_type=jnp.float32)
        taps_grad = jnp.fft.irfft(signal_spec * jnp.conj(value_spec), n=fft_len, axis=1)[:, :seq_len]
        rms = jnp.sqrt(jnp.mean(taps_grad * taps_grad) + 1e-06)
        factor = jnp.minimum(1.0, bound_raw.astype(jnp.float32) / rms)
        return (running + factor * taps_grad, input_grad.astype(jnp.bfloat16))
    start_sum = jnp.zeros(filter_taps.shape, jnp.float32)
    filter_grad, input_grad = lax.scan(one_example, start_sum, (stream, cotangent, base_ids, clip_bound))
    return (input_grad, filter_grad)
```

```python
import functools
import math

import jax
import jax.numpy as jnp
import numpy as np
from jax import lax
from jax.experimental import pallas as pl
from jax.experimental.pallas import tpu as pltpu
from jax.sharding import PartitionSpec as P


LANES = 128
BLOCKS = 256
SEQ = LANES * BLOCKS
UNKNOWN_BASE = 4
NORM_EPS = 1e-06

f32 = jnp.float32
bf16 = jnp.bfloat16


def tables():
    row = np.arange(BLOCKS, dtype=np.float64)
    lane = np.arange(LANES, dtype=np.float64)
    first = 2.0 * np.pi * np.outer(row + 0.25, row) / BLOCKS
    fwd_rows = np.concatenate([np.cos(first), -np.sin(first)], axis=0)
    inv_rows = np.concatenate([np.cos(first.T), -np.sin(first.T)], axis=1) / SEQ
    twist = 2.0 * np.pi * np.outer(row + 0.25, lane) / SEQ
    second = 2.0 * np.pi * (np.outer(lane, lane) % LANES) / LANES
    cos2, sin2 = np.cos(second), np.sin(second)
    fwd_lanes = np.block([[cos2, -sin2], [sin2, cos2]])
    inv_lanes = np.block([[cos2, sin2], [-sin2, cos2]])
    half = lambda table: jnp.asarray(table.astype(np.float32)).astype(bf16)
    return (
        half(fwd_rows),
        half(fwd_lanes),
        half(inv_lanes),
        half(inv_rows),
        jnp.asarray(np.cos(twist).astype(np.float32)),
        jnp.asarray(np.sin(twist).astype(np.float32)),
    )


def mm(a, b):
    return jnp.dot(a, b, preferred_element_type=f32)


def project_kernel(x_ref, cot_ref, ids_ref, wv_ref, wg_ref, out_ref):
    groups = out_ref.shape[0]
    width = 2 * LANES
    for step in range(x_ref.shape[1] // width):
        cols = slice(step * width, (step + 1) * width)
        tokens = x_ref[:, cols]
        value = mm(wv_ref[...], tokens)
        gate = mm(wg_ref[...], tokens).astype(bf16).astype(f32)
        keep = jnp.where(ids_ref[:, cols] != UNKNOWN_BASE, 1.0, 0.0)
        signal = gate * (cot_ref[:, cols].astype(f32) * keep)
        for side in range(2):
            lanes = slice(side * LANES, (side + 1) * LANES)
            both = jnp.concatenate(
                [
                    value[:, lanes].reshape(groups, 8, LANES),
                    signal[:, lanes].reshape(groups, 8, LANES),
                ],
                axis=1,
            )
            out_ref[:, 2 * step + side] = both.astype(bf16)


def forward(two, fwd_rows, fwd_lanes, cos_t, sin_t):
    first = mm(fwd_rows[...], two)
    outs = []
    for side in range(2):
        re = first[:BLOCKS, side * LANES : (side + 1) * LANES]
        im = first[BLOCKS:, side * LANES : (side + 1) * LANES]
        cos_v, sin_v = cos_t[...], sin_t[...]
        turned = jnp.concatenate(
            [
                (re * cos_v + im * sin_v).astype(bf16),
                (im * cos_v - re * sin_v).astype(bf16),
            ],
            axis=1,
        )
        outs.append(mm(turned, fwd_lanes[...]))
    return outs


def inverse(pair, inv_lanes, inv_rows, cos_t, sin_t):
    res, ims = [], []
    for spectrum in pair:
        mid = mm(spectrum, inv_lanes[...])
        re, im = mid[:, :LANES], mid[:, LANES:]
        cos_v, sin_v = cos_t[...], sin_t[...]
        res.append((re * cos_v - im * sin_v).astype(bf16))
        ims.append((im * cos_v + re * sin_v).astype(bf16))
    stacked = jnp.concatenate(
        [jnp.concatenate(res, axis=1), jnp.concatenate(ims, axis=1)], axis=0
    )
    return mm(inv_rows[...], stacked)


def taps_grad_kernel(
    seq_ref, fr_ref, fl_ref, il_ref, ir_ref, ct_ref, st_ref,
    grad_ref, sum_ref, chan_ref, val_ref, sig_ref, wide_ref,
):
    wide_ref[...] = seq_ref[...].astype(f32).reshape(wide_ref.shape)
    stride = seq_ref.shape[1]
    channels = stride // 2

    def pair_step(step, total):
        spectra = []
        for kind, keep_ref in ((0, val_ref), (1, sig_ref)):
            halves = []
            for side in range(2):
                row = kind * channels + 2 * step + side
                part = wide_ref[pl.ds(row, BLOCKS, stride=stride), :].astype(bf16)
                chan_ref[row] = part
                halves.append(part)
            both = forward(jnp.concatenate(halves, axis=1), fr_ref, fl_ref, ct_ref, st_ref)
            for side in range(2):
                keep_ref[2 * step + side] = both[side]
            spectra.append(both)
        products = []
        for side in range(2):
            vr, vi = spectra[0][side][:, :LANES], spectra[0][side][:, LANES:]
            sr, si = spectra[1][side][:, :LANES], spectra[1][side][:, LANES:]
            products.append(
                jnp.concatenate(
                    [(sr * vr + si * vi).astype(bf16), (si * vr - sr * vi).astype(bf16)], axis=1
                )
            )
        both = inverse(products, il_ref, ir_ref, ct_ref, st_ref)
        for side in range(2):
            grad = both[:, side * LANES : (side + 1) * LANES]
            grad_ref[pl.ds(2 * step + side, BLOCKS, stride=channels), :] = grad
        return total + jnp.sum((both * both).reshape(-1, 8, 2 * LANES), axis=0)

    total = lax.fori_loop(0, channels // 2, pair_step, jnp.zeros((8, 2 * LANES), f32))
    sum_ref[...] = jnp.broadcast_to(jnp.sum(total), sum_ref.shape)


def lag_tiles(by_lag_ref, channels):
    per_owner = by_lag_ref.shape[2] // LANES
    for block in range(by_lag_ref.shape[0] * per_owner):
        owner, inner = divmod(block, per_owner)
        rows = slice(block * channels, (block + 1) * channels)
        yield owner, slice(inner * LANES, (inner + 1) * LANES), rows


def scatter_lags(wide_ref, by_lag_ref, channels):
    for owner, lanes, rows in lag_tiles(by_lag_ref, channels):
        wide_ref[rows] = by_lag_ref[owner, :, lanes]


def state_kernel(
    bias_ref, taps_ref, val_ref, sig_ref, chan_ref, fr_ref, fl_ref, il_ref, ir_ref, ct_ref, st_ref,
    out_ref, taps_wide_ref, wide_ref,
):
    stride = out_ref.shape[1]
    channels = stride // 2
    scatter_lags(taps_wide_ref, taps_ref, channels)

    def pair_step(step, carry):
        halves = []
        for side in range(2):
            rows = pl.ds(2 * step + side, BLOCKS, stride=channels)
            halves.append(taps_wide_ref[rows, :].astype(bf16))
        filt = forward(jnp.concatenate(halves, axis=1), fr_ref, fl_ref, ct_ref, st_ref)
        for kind, spec_ref in ((1, val_ref), (0, sig_ref)):
            products = []
            for side in range(2):
                hr, hi = filt[side][:, :LANES], filt[side][:, LANES:]
                other = spec_ref[2 * step + side]
                xr, xi = other[:, :LANES], other[:, LANES:]
                if kind == 1:
                    re, im = hr * xr - hi * xi, hr * xi + hi * xr
                else:
                    re, im = hr * xr + hi * xi, hr * xi - hi * xr
                products.append(jnp.concatenate([re.astype(bf16), im.astype(bf16)], axis=1))
            both = inverse(products, il_ref, ir_ref, ct_ref, st_ref)
            for side in range(2):
                chan = 2 * step + side
                direct = bias_ref[chan] * chan_ref[(1 - kind) * channels + chan].astype(f32)
                rows = pl.ds(kind * channels + chan, BLOCKS, stride=stride)
                wide_ref[rows, :] = both[:, side * LANES : (side + 1) * LANES] + direct
        return carry

    lax.fori_loop(0, channels // 2, pair_step, 0)
    out_ref[...] = wide_ref[...].reshape(out_ref.shape).astype(bf16)


def scale_kernel(clip_ref, parts_ref, grad_ref, out_ref, *, entries):
    total = jnp.sum(parts_ref[...], axis=0)
    bound = clip_ref[0].astype(f32)
    factor = jnp.minimum(1.0, bound / jnp.sqrt(total / entries + NORM_EPS))
    for owner, lanes, rows in lag_tiles(out_ref, out_ref.shape[1]):
        out_ref[owner, :, lanes] = grad_ref[rows] * factor


def input_grad_kernel(recv_ref, cot_ref, ids_ref, wv_ref, wg_ref, out_ref):
    width = 2 * LANES
    for step in range(cot_ref.shape[1] // width):
        cols = slice(step * width, (step + 1) * width)
        keep = jnp.where(ids_ref[:, cols] != UNKNOWN_BASE, 1.0, 0.0)
        cot = cot_ref[:, cols].astype(f32) * keep
        grads, states = [], []
        for side in range(2):
            both = recv_ref[:, 2 * step + side].astype(f32)
            grads.append(both[:, :8].reshape(-1, LANES))
            states.append(both[:, 8:].reshape(-1, LANES))
        grad = jnp.concatenate(grads, axis=1).astype(bf16)
        gated = (jnp.concatenate(states, axis=1) * cot).astype(bf16)
        out_ref[:, cols] = (mm(wv_ref[...], grad) + mm(wg_ref[...], gated)).astype(bf16)


VMEM = pl.BlockSpec(memory_space=pltpu.VMEM)
SMEM = pl.BlockSpec(memory_space=pltpu.SMEM)


def call(body, outs, args, scratch=(), scalars=0, flops=0, limit=16):
    specs = [SMEM] * scalars + [VMEM] * (len(args) - scalars)
    single = not isinstance(outs, (tuple, list))
    size = sum(math.prod(o.shape) * o.dtype.itemsize for o in ([outs] if single else outs))
    return pl.pallas_call(
        body,
        out_shape=outs,
        in_specs=specs,
        out_specs=VMEM if single else tuple(VMEM for _ in outs),
        scratch_shapes=list(scratch),
        cost_estimate=pl.CostEstimate(flops=flops, transcendentals=0, bytes_accessed=2 * size),
        compiler_params=pltpu.CompilerParams(vmem_limit_bytes=limit * 1024 * 1024),
    )(*args)


def exchange(x, axis):
    return lax.all_to_all(x, axis, 0, 0, tiled=True)


def step(stream, cotangent, base_ids, clip_bound, w_value, w_gate, filter_taps, filter_bias):
    n_ctx, n_ex = lax.axis_size("ctx"), lax.axis_size("ex")
    width, tokens = stream.shape[1:]
    channels = filter_taps.shape[0]
    blocks = tokens // LANES
    shape = jax.ShapeDtypeStruct
    tabs = tables()

    sent = call(
        project_kernel, shape((n_ctx, blocks, 2 * channels, LANES), bf16),
        (stream[0], cotangent[0], base_ids, w_value, w_gate), flops=4 * width * width * tokens,
    )
    seqs = exchange(sent, "ctx").reshape(BLOCKS, 2 * channels, LANES)
    taps = lax.all_gather(filter_taps, "ex", axis=0)
    grad, part, chans, val_spec, sig_spec = call(
        taps_grad_kernel,
        (
            shape((BLOCKS * channels, LANES), f32),
            shape((n_ctx, 1, LANES), f32),
            shape((2 * channels, BLOCKS, LANES), bf16),
            shape((channels, BLOCKS, 2 * LANES), f32),
            shape((channels, BLOCKS, 2 * LANES), f32),
        ),
        (seqs, *tabs),
        scratch=[pltpu.VMEM((BLOCKS * 2 * channels, LANES), f32)],
        flops=3 * 2 * 2 * channels * 512 * 256 * 128, limit=24,
    )
    parts = exchange(part, "ctx")
    outs = call(
        state_kernel, shape((BLOCKS, 2 * channels, LANES), bf16),
        (filter_bias, taps, val_spec, sig_spec, chans, *tabs),
        scratch=[
            pltpu.VMEM((BLOCKS * channels, LANES), f32),
            pltpu.VMEM((BLOCKS * 2 * channels, LANES), f32),
        ],
        scalars=1, flops=3 * 2 * 2 * channels * 512 * 256 * 128, limit=24,
    )
    back = exchange(outs.reshape(n_ctx, blocks, 2 * channels, LANES), "ctx")
    scaled = call(
        functools.partial(scale_kernel, entries=float(tokens * n_ctx * width)),
        shape((n_ex, *filter_taps.shape), f32), (clip_bound, parts, grad), scalars=1,
    )
    filter_grad = lax.psum_scatter(scaled, "ex", scatter_dimension=0)
    input_grad = call(
        input_grad_kernel, shape((width, tokens), bf16),
        (back, cotangent[0], base_ids, w_value.T, w_gate.T), flops=4 * width * width * tokens,
    )
    return (input_grad[None], filter_grad)


def solution(mesh):
    in_specs = (
        P("ex", None, "ctx"),
        P("ex", None, "ctx"),
        P("ex", "ctx"),
        P("ex"),
        P(),
        P(),
        P("ctx", "ex"),
        P("ctx"),
    )
    out_specs = (P("ex", None, "ctx"), P("ctx", "ex"))
    return jax.shard_map(step, mesh=mesh, in_specs=in_specs, out_specs=out_specs, check_vma=False)
```

```python
import functools
import math

import jax
import jax.numpy as jnp
import numpy as np
from jax import lax
from jax.experimental import pallas as pl
from jax.experimental.pallas import tpu as pltpu
from jax.sharding import PartitionSpec as P


LANES = 128
BLOCKS = 256
SEQ = LANES * BLOCKS
N_EX = 8
SEND_ORDER = (0, 1, 7, 2, 6, 3, 5, 4)
UNKNOWN_BASE = 4
NORM_EPS = 1e-06

f32 = jnp.float32
bf16 = jnp.bfloat16


def tables():
    row = np.arange(BLOCKS, dtype=np.float64)
    lane = np.arange(LANES, dtype=np.float64)
    first = 2.0 * np.pi * np.outer(row + 0.25, row) / BLOCKS
    fwd_rows = np.concatenate([np.cos(first), -np.sin(first)], axis=0)
    inv_rows = np.concatenate([np.cos(first.T), -np.sin(first.T)], axis=1) / SEQ
    twist = 2.0 * np.pi * np.outer(row + 0.25, lane) / SEQ
    second = 2.0 * np.pi * (np.outer(lane, lane) % LANES) / LANES
    cos2, sin2 = np.cos(second), np.sin(second)
    fwd_lanes = np.block([[cos2, -sin2], [sin2, cos2]])
    inv_lanes = np.block([[cos2, sin2], [-sin2, cos2]])
    half = lambda table: jnp.asarray(table.astype(np.float32)).astype(bf16)
    return (
        half(fwd_rows),
        half(fwd_lanes),
        half(inv_lanes),
        half(inv_rows),
        jnp.asarray(np.cos(twist).astype(np.float32)),
        jnp.asarray(np.sin(twist).astype(np.float32)),
    )


def mm(a, b):
    return jnp.dot(a, b, preferred_element_type=f32)


def start_all(copies):
    for copy in copies:
        copy.start()


def wait_all(copies):
    for copy in copies:
        copy.wait()


def project_kernel(
    x_hbm, cot_hbm, ids_hbm, wv_hbm, wg_hbm, out_hbm,
    x_ref, cot_ref, ids_ref, wv_ref, wg_ref, out_ref, sems,
):
    groups = out_ref.shape[0]
    width = 2 * LANES
    steps = x_ref.shape[1] // width
    copy = pltpu.make_async_copy
    shared = [
        copy(wv_hbm, wv_ref, sems.at[0]),
        copy(wg_hbm, wg_ref, sems.at[1]),
        copy(ids_hbm, ids_ref, sems.at[2]),
    ]
    ins, outs = [], []
    for step in range(steps):
        cols = pl.ds(step * width, width)
        ins.append(
            (
                copy(x_hbm.at[:, cols], x_ref.at[:, cols], sems.at[3 + step]),
                copy(cot_hbm.at[:, cols], cot_ref.at[:, cols], sems.at[3 + steps + step]),
            )
        )
        pair = pl.ds(2 * step, 2)
        outs.append(copy(out_ref.at[:, pair], out_hbm.at[:, pair], sems.at[3 + 2 * steps + step]))
    start_all(shared)
    for both in ins:
        start_all(both)
    wait_all(shared)
    for step in range(steps):
        wait_all(ins[step])
        cols = slice(step * width, (step + 1) * width)
        tokens = x_ref[:, cols]
        value = mm(wv_ref[...], tokens)
        gate = mm(wg_ref[...], tokens).astype(bf16).astype(f32)
        keep = jnp.where(ids_ref[:, cols] != UNKNOWN_BASE, 1.0, 0.0)
        signal = gate * (cot_ref[:, cols].astype(f32) * keep)
        for side in range(2):
            lanes = slice(side * LANES, (side + 1) * LANES)
            both = jnp.concatenate(
                [
                    value[:, lanes].reshape(groups, 8, LANES),
                    signal[:, lanes].reshape(groups, 8, LANES),
                ],
                axis=1,
            )
            out_ref[:, 2 * step + side] = both.astype(bf16)
        outs[step].start()
    wait_all(outs)


def forward(two, fwd_rows, fwd_lanes, cos_t, sin_t):
    first = mm(fwd_rows[...], two)
    outs = []
    for side in range(2):
        re = first[:BLOCKS, side * LANES : (side + 1) * LANES]
        im = first[BLOCKS:, side * LANES : (side + 1) * LANES]
        cos_v, sin_v = cos_t[...], sin_t[...]
        turned = jnp.concatenate(
            [
                (re * cos_v + im * sin_v).astype(bf16),
                (im * cos_v - re * sin_v).astype(bf16),
            ],
            axis=1,
        )
        outs.append(mm(turned, fwd_lanes[...]))
    return outs


def inverse(pair, inv_lanes, inv_rows, cos_t, sin_t):
    res, ims = [], []
    for spectrum in pair:
        mid = mm(spectrum, inv_lanes[...])
        re, im = mid[:, :LANES], mid[:, LANES:]
        cos_v, sin_v = cos_t[...], sin_t[...]
        res.append((re * cos_v - im * sin_v).astype(bf16))
        ims.append((im * cos_v + re * sin_v).astype(bf16))
    stacked = jnp.concatenate(
        [jnp.concatenate(res, axis=1), jnp.concatenate(ims, axis=1)], axis=0
    )
    return mm(inv_rows[...], stacked)


TABLE_SHAPES = (
    ((2 * BLOCKS, BLOCKS), bf16),
    ((2 * LANES, 2 * LANES), bf16),
    ((2 * LANES, 2 * LANES), bf16),
    ((BLOCKS, 2 * BLOCKS), bf16),
    ((BLOCKS, LANES), f32),
    ((BLOCKS, LANES), f32),
)
N_TABLES = len(TABLE_SHAPES)
CHUNKS = 4


def table_copies(hbm_refs, refs, sems):
    return [pltpu.make_async_copy(h, v, sems.at[i]) for i, (h, v) in enumerate(zip(hbm_refs, refs))]


def taps_grad_kernel(*refs):
    seq_hbm, tabs_hbm = refs[0], refs[1 : 1 + N_TABLES]
    grad_hbm, sum_hbm, chan_hbm, val_hbm, sig_hbm = refs[1 + N_TABLES : 6 + N_TABLES]
    rest = refs[6 + N_TABLES :]
    tabs, rest = rest[:N_TABLES], rest[N_TABLES:]
    seq_ref, wide_ref, grad_ref, sum_ref, chan_ref, val_ref, sig_ref, tab_sems, seq_sems, out_sems = rest
    fr_ref, fl_ref, il_ref, ir_ref, ct_ref, st_ref = tabs
    copy = pltpu.make_async_copy
    stride = seq_ref.shape[1]
    channels = stride // 2
    part = BLOCKS // CHUNKS
    seq_copies = [
        copy(seq_hbm.at[pl.ds(i * part, part)], seq_ref.at[pl.ds(i * part, part)], seq_sems.at[i])
        for i in range(CHUNKS)
    ]
    tab_copies = table_copies(tabs_hbm, tabs, tab_sems)
    start_all(seq_copies)
    start_all(tab_copies)
    for i in range(CHUNKS):
        seq_copies[i].wait()
        rows = seq_ref[i * part : (i + 1) * part].astype(f32).reshape(part * stride, LANES)
        wide_ref[i * part * stride : (i + 1) * part * stride] = rows
    wait_all(tab_copies)

    def out_copies(step):
        pair = pl.ds(2 * step, 2)
        second = pl.ds(channels + 2 * step, 2)
        return [
            copy(val_ref.at[pair], val_hbm.at[pair], out_sems.at[0, step]),
            copy(sig_ref.at[pair], sig_hbm.at[pair], out_sems.at[1, step]),
            copy(chan_ref.at[pair], chan_hbm.at[pair], out_sems.at[2, step]),
            copy(chan_ref.at[second], chan_hbm.at[second], out_sems.at[3, step]),
            copy(grad_ref.at[pair], grad_hbm.at[pair], out_sems.at[4, step]),
        ]

    def pair_step(step, total):
        spectra = []
        for kind, keep_ref in ((0, val_ref), (1, sig_ref)):
            halves = []
            for side in range(2):
                row = kind * channels + 2 * step + side
                piece = wide_ref[pl.ds(row, BLOCKS, stride=stride), :].astype(bf16)
                chan_ref[row] = piece
                halves.append(piece)
            both = forward(jnp.concatenate(halves, axis=1), fr_ref, fl_ref, ct_ref, st_ref)
            for side in range(2):
                keep_ref[2 * step + side] = both[side]
            spectra.append(both)
        products = []
        for side in range(2):
            vr, vi = spectra[0][side][:, :LANES], spectra[0][side][:, LANES:]
            sr, si = spectra[1][side][:, :LANES], spectra[1][side][:, LANES:]
            products.append(
                jnp.concatenate(
                    [(sr * vr + si * vi).astype(bf16), (si * vr - sr * vi).astype(bf16)], axis=1
                )
            )
        both = inverse(products, il_ref, ir_ref, ct_ref, st_ref)
        for side in range(2):
            grad_ref[2 * step + side] = both[:, side * LANES : (side + 1) * LANES]
        start_all(out_copies(step))
        return total + jnp.sum((both * both).reshape(-1, 8, 2 * LANES), axis=0)

    total = lax.fori_loop(0, channels // 2, pair_step, jnp.zeros((8, 2 * LANES), f32))
    sum_ref[...] = jnp.broadcast_to(jnp.sum(total), sum_ref.shape)
    last = copy(sum_ref, sum_hbm, seq_sems.at[CHUNKS])
    last.start()
    for step in range(channels // 2):
        wait_all(out_copies(step))
    last.wait()


def state_kernel(*refs):
    bias_ref, refs = refs[0], refs[1:]
    taps_hbm, refs = refs[:N_EX], refs[N_EX:]
    val_hbm, sig_hbm, chan_hbm, refs = *refs[:3], refs[3:]
    tabs_hbm, out_hbm, refs = refs[:N_TABLES], refs[N_TABLES], refs[N_TABLES + 1 :]
    tabs, refs = refs[:N_TABLES], refs[N_TABLES:]
    taps_ref, taps_wide_ref, val_ref, sig_ref, chan_ref, wide_ref, out_ref = refs[:7]
    tab_sems, taps_sems, in_sems, out_sems = refs[7:]
    fr_ref, fl_ref, il_ref, ir_ref, ct_ref, st_ref = tabs
    copy = pltpu.make_async_copy
    stride = out_ref.shape[1]
    channels = stride // 2

    def in_copies(step):
        pair = pl.ds(2 * step, 2)
        second = pl.ds(channels + 2 * step, 2)
        return [
            copy(val_hbm.at[pair], val_ref.at[pair], in_sems.at[0, step]),
            copy(sig_hbm.at[pair], sig_ref.at[pair], in_sems.at[1, step]),
            copy(chan_hbm.at[pair], chan_ref.at[pair], in_sems.at[2, step]),
            copy(chan_hbm.at[second], chan_ref.at[second], in_sems.at[3, step]),
        ]

    taps_copies = [copy(taps_hbm[k], taps_ref.at[k], taps_sems.at[k]) for k in range(N_EX)]
    tab_copies = table_copies(tabs_hbm, tabs, tab_sems)
    start_all(taps_copies)
    start_all(tab_copies)
    for step in range(channels // 2):
        start_all(in_copies(step))
    place = lax.axis_index("ex")
    own_blocks = BLOCKS // N_EX
    for k in range(N_EX):
        taps_copies[k].wait()
        base = lax.rem(place + (N_EX - k), N_EX) * (own_blocks * channels)
        for block in range(own_blocks):
            rows = pl.ds(pl.multiple_of(base + block * channels, channels), channels)
            taps_wide_ref[rows, :] = taps_ref[k, :, block * LANES : (block + 1) * LANES].astype(f32)
    wait_all(tab_copies)

    def pair_step(step, carry):
        halves = []
        for side in range(2):
            rows = pl.ds(2 * step + side, BLOCKS, stride=channels)
            halves.append(taps_wide_ref[rows, :].astype(bf16))
        filt = forward(jnp.concatenate(halves, axis=1), fr_ref, fl_ref, ct_ref, st_ref)
        wait_all(in_copies(step))
        for kind, spec_ref in ((1, val_ref), (0, sig_ref)):
            products = []
            for side in range(2):
                hr, hi = filt[side][:, :LANES], filt[side][:, LANES:]
                other = spec_ref[2 * step + side]
                xr, xi = other[:, :LANES], other[:, LANES:]
                if kind == 1:
                    re, im = hr * xr - hi * xi, hr * xi + hi * xr
                else:
                    re, im = hr * xr + hi * xi, hr * xi - hi * xr
                products.append(jnp.concatenate([re.astype(bf16), im.astype(bf16)], axis=1))
            both = inverse(products, il_ref, ir_ref, ct_ref, st_ref)
            for side in range(2):
                chan = 2 * step + side
                direct = bias_ref[chan] * chan_ref[(1 - kind) * channels + chan].astype(f32)
                rows = pl.ds(kind * channels + chan, BLOCKS, stride=stride)
                wide_ref[rows, :] = both[:, side * LANES : (side + 1) * LANES] + direct
        return carry

    lax.fori_loop(0, channels // 2, pair_step, 0)
    part = BLOCKS // CHUNKS
    outs = []
    for i in range(CHUNKS):
        rows = wide_ref[i * part * stride : (i + 1) * part * stride]
        out_ref[i * part : (i + 1) * part] = rows.reshape(part, stride, LANES).astype(bf16)
        span = pl.ds(i * part, part)
        outs.append(copy(out_ref.at[span], out_hbm.at[span], out_sems.at[i]))
        outs[i].start()
    wait_all(outs)


def scale_kernel(clip_ref, *refs, entries):
    parts_hbm, grad_hbm, refs = refs[0], refs[1], refs[2:]
    out_hbm, (parts_ref, grad_ref, out_ref, in_sems, out_sems) = refs[:N_EX], refs[N_EX:]
    copy = pltpu.make_async_copy
    own = BLOCKS // N_EX
    ins = [
        copy(parts_hbm, parts_ref, in_sems.at[0]),
        copy(grad_hbm, grad_ref, in_sems.at[1]),
    ]
    start_all(ins)
    wait_all(ins)
    total = jnp.sum(parts_ref[...], axis=0)
    bound = clip_ref[0].astype(f32)
    factor = jnp.minimum(1.0, bound / jnp.sqrt(total / entries + NORM_EPS))
    place = lax.axis_index("ex")
    outs = []
    for k in SEND_ORDER:
        base = pl.multiple_of(lax.rem(place + k, N_EX) * own, own)
        out_ref[k] = (grad_ref[:, pl.ds(base, own), :] * factor).astype(bf16)
        outs.append(copy(out_ref.at[k], out_hbm[k], out_sems.at[k]))
        outs[-1].start()
    wait_all(outs)


def input_grad_kernel(
    recv_hbm, cot_hbm, ids_hbm, wv_hbm, wg_hbm, out_hbm,
    recv_ref, cot_ref, ids_ref, wv_ref, wg_ref, out_ref, sems,
):
    width = 2 * LANES
    steps = cot_ref.shape[1] // width
    copy = pltpu.make_async_copy
    shared = [
        copy(wv_hbm, wv_ref, sems.at[0]),
        copy(wg_hbm, wg_ref, sems.at[1]),
        copy(ids_hbm, ids_ref, sems.at[2]),
    ]
    ins, outs = [], []
    for step in range(steps):
        cols, pair = pl.ds(step * width, width), pl.ds(2 * step, 2)
        ins.append(
            (
                copy(recv_hbm.at[:, pair], recv_ref.at[:, pair], sems.at[3 + step]),
                copy(cot_hbm.at[:, cols], cot_ref.at[:, cols], sems.at[3 + steps + step]),
            )
        )
        outs.append(
            copy(out_ref.at[:, cols], out_hbm.at[:, cols], sems.at[3 + 2 * steps + step])
        )
    start_all(shared)
    for both in ins:
        start_all(both)
    wait_all(shared)
    for step in range(steps):
        wait_all(ins[step])
        cols = slice(step * width, (step + 1) * width)
        keep = jnp.where(ids_ref[:, cols] != UNKNOWN_BASE, 1.0, 0.0)
        cot = cot_ref[:, cols].astype(f32) * keep
        grads, states = [], []
        for side in range(2):
            both = recv_ref[:, 2 * step + side].astype(f32)
            grads.append(both[:, :8].reshape(-1, LANES))
            states.append(both[:, 8:].reshape(-1, LANES))
        grad = jnp.concatenate(grads, axis=1).astype(bf16)
        gated = (jnp.concatenate(states, axis=1) * cot).astype(bf16)
        out_ref[:, cols] = (mm(wv_ref[...], grad) + mm(wg_ref[...], gated)).astype(bf16)
        outs[step].start()
    wait_all(outs)


def combine_kernel(*refs):
    recv_hbm, out_hbm = refs[:N_EX], refs[N_EX]
    recv_ref, total_ref, out_ref, sems = refs[N_EX + 1 :]
    copy = pltpu.make_async_copy
    ins = [copy(recv_hbm[k], recv_ref.at[k], sems.at[k]) for k in range(N_EX)]
    start_all(ins)
    wait_all(ins)
    total = jnp.sum(recv_ref[...].astype(f32), axis=0)
    channels, blocks = total.shape[:2]
    total_ref[...] = total.reshape(total_ref.shape)
    for block in range(blocks):
        lanes = slice(block * LANES, (block + 1) * LANES)
        out_ref[:, lanes] = total_ref[pl.ds(block, channels, stride=blocks), :]
    last = copy(out_ref, out_hbm, sems.at[N_EX])
    last.start()
    last.wait()


HBM = pl.BlockSpec(memory_space=pltpu.HBM)
SMEM = pl.BlockSpec(memory_space=pltpu.SMEM)


def call(body, outs, args, scratch, scalars=0, flops=0, limit=67043328):
    specs = [SMEM] * scalars + [HBM] * (len(args) - scalars)
    single = not isinstance(outs, (tuple, list))
    size = sum(math.prod(o.shape) * o.dtype.itemsize for o in ([outs] if single else outs))
    return pl.pallas_call(
        body,
        out_shape=outs,
        in_specs=specs,
        out_specs=HBM if single else tuple(HBM for _ in outs),
        scratch_shapes=list(scratch),
        cost_estimate=pl.CostEstimate(flops=flops, transcendentals=0, bytes_accessed=2 * size),
        compiler_params=pltpu.CompilerParams(vmem_limit_bytes=limit),
    )(*args)


def exchange(x, axis):
    return lax.all_to_all(x, axis, 0, 0, tiled=True)


def shift(x, places):
    ring = [(i, (i + places) % N_EX) for i in range(N_EX)]
    return lax.ppermute(x, "ex", ring)


def step(stream, cotangent, base_ids, clip_bound, w_value, w_gate, filter_taps, filter_bias):
    n_ctx = lax.axis_size("ctx")
    width, tokens = stream.shape[1:]
    channels = filter_taps.shape[0]
    blocks = tokens // LANES
    shape, vmem, dma = jax.ShapeDtypeStruct, pltpu.VMEM, pltpu.SemaphoreType.DMA
    tabs = tables()
    tab_scratch = [vmem(*s) for s in TABLE_SHAPES]
    pairs = channels // 2
    steps = blocks // 2
    transform = 2 * 2 * channels * 512 * 256 * 128
    token_scratch = [
        vmem((width, tokens), bf16),
        vmem(base_ids.shape, jnp.int32),
        vmem((width, width), bf16),
        vmem((width, width), bf16),
    ]
    message = (n_ctx, blocks, 2 * channels, LANES)

    own_taps = filter_taps.astype(bf16)
    sent = call(
        project_kernel, shape(message, bf16),
        (stream[0], cotangent[0], base_ids, w_value, w_gate),
        [vmem((width, tokens), bf16), *token_scratch, vmem(message, bf16), dma((3 + 3 * steps,))],
        flops=4 * width * width * tokens,
    )
    seqs = exchange(sent, "ctx").reshape(BLOCKS, 2 * channels, LANES)
    taps = [own_taps] + [None] * (N_EX - 1)
    for k in SEND_ORDER[1:]:
        taps[k] = shift(own_taps, k)

    by_channel = (channels, BLOCKS, LANES)
    spectrum = (channels, BLOCKS, 2 * LANES)
    both_chans = (2 * channels, BLOCKS, LANES)
    both_seqs = (BLOCKS, 2 * channels, LANES)
    grad, part, chans, val_spec, sig_spec = call(
        taps_grad_kernel,
        (
            shape(by_channel, f32),
            shape((n_ctx, 1, LANES), f32),
            shape(both_chans, bf16),
            shape(spectrum, f32),
            shape(spectrum, f32),
        ),
        (seqs, *tabs),
        [
            *tab_scratch,
            vmem(both_seqs, bf16),
            vmem((BLOCKS * 2 * channels, LANES), f32),
            vmem(by_channel, f32),
            vmem((n_ctx, 1, LANES), f32),
            vmem(both_chans, bf16),
            vmem(spectrum, f32),
            vmem(spectrum, f32),
            dma((N_TABLES,)),
            dma((CHUNKS + 1,)),
            dma((5, pairs)),
        ],
        flops=3 * transform,
    )
    parts = exchange(part, "ctx")
    outs = call(
        state_kernel, shape(both_seqs, bf16),
        (filter_bias, *taps, val_spec, sig_spec, chans, *tabs),
        [
            *tab_scratch,
            vmem((N_EX, *filter_taps.shape), bf16),
            vmem((BLOCKS * channels, LANES), f32),
            vmem(spectrum, f32),
            vmem(spectrum, f32),
            vmem(both_chans, bf16),
            vmem((BLOCKS * 2 * channels, LANES), f32),
            vmem(both_seqs, bf16),
            dma((N_TABLES,)),
            dma((N_EX,)),
            dma((4, pairs)),
            dma((CHUNKS,)),
        ],
        scalars=1, flops=3 * transform,
    )
    back = exchange(outs.reshape(message), "ctx")
    piece = (channels, BLOCKS // N_EX, LANES)
    scaled = call(
        functools.partial(scale_kernel, entries=float(tokens * n_ctx * width)),
        tuple(shape(piece, bf16) for _ in range(N_EX)), (clip_bound, parts, grad),
        [
            vmem((n_ctx, 1, LANES), f32),
            vmem(by_channel, f32),
            vmem((N_EX, *piece), bf16),
            dma((2,)),
            dma((N_EX,)),
        ],
        scalars=1,
    )
    owned = [scaled[0]] + [None] * (N_EX - 1)
    for k in SEND_ORDER[1:]:
        owned[k] = shift(scaled[k], k)
    input_grad = call(
        input_grad_kernel, shape((width, tokens), bf16),
        (back, cotangent[0], base_ids, w_value.T, w_gate.T),
        [vmem(message, bf16), *token_scratch, vmem((width, tokens), bf16), dma((3 + 3 * steps,))],
        flops=4 * width * width * tokens,
    )
    filter_grad = call(
        combine_kernel, shape(filter_taps.shape, f32), tuple(owned),
        [
            vmem((N_EX, *piece), bf16),
            vmem((channels * piece[1], LANES), f32),
            vmem(filter_taps.shape, f32),
            dma((N_EX + 1,)),
        ],
    )
    return (input_grad[None], filter_grad)


def solution(mesh):
    in_specs = (
        P("ex", None, "ctx"),
        P("ex", None, "ctx"),
        P("ex", "ctx"),
        P("ex"),
        P(),
        P(),
        P("ctx", "ex"),
        P("ctx"),
    )
    out_specs = (P("ex", None, "ctx"), P("ctx", "ex"))
    return jax.shard_map(step, mesh=mesh, in_specs=in_specs, out_specs=out_specs, check_vma=False)
```

```python
import math

import jax
import jax.numpy as jnp
import numpy as np
from jax import lax
from jax.experimental import pallas as pl
from jax.experimental.pallas import tpu as pltpu
from jax.sharding import PartitionSpec as P


LANES = 128
BLOCKS = 256
SEQ = LANES * BLOCKS
N_EX = 8
SEND_ORDER = (0, 1, 7, 2, 6, 3, 5, 4)
RELAYS = ((1, 0, 1), (7, 0, 7), (2, 0, 2), (6, 0, 6), (3, 1, 2), (5, 7, 6), (4, 2, 2))
UNKNOWN_BASE = 4
NORM_EPS = 1e-06

f32 = jnp.float32
bf16 = jnp.bfloat16


def tables():
    row = np.arange(BLOCKS, dtype=np.float64)
    lane = np.arange(LANES, dtype=np.float64)
    first = 2.0 * np.pi * np.outer(row + 0.25, row) / BLOCKS
    fwd_rows = np.concatenate([np.cos(first), -np.sin(first)], axis=0)
    inv_rows = np.concatenate([np.cos(first.T), -np.sin(first.T)], axis=1) / SEQ
    twist = 2.0 * np.pi * np.outer(row + 0.25, lane) / SEQ
    second = 2.0 * np.pi * (np.outer(lane, lane) % LANES) / LANES
    cos2, sin2 = np.cos(second), np.sin(second)
    fwd_lanes = np.block([[cos2, -sin2], [sin2, cos2]])
    inv_lanes = np.block([[cos2, sin2], [-sin2, cos2]])
    half = lambda table: jnp.asarray(table.astype(np.float32)).astype(bf16)
    return (
        half(fwd_rows),
        half(fwd_lanes),
        half(inv_lanes),
        half(inv_rows),
        jnp.asarray(np.cos(twist).astype(np.float32)),
        jnp.asarray(np.sin(twist).astype(np.float32)),
    )


def mm(a, b):
    return jnp.dot(a, b, preferred_element_type=f32)


def start_all(copies):
    for copy in copies:
        copy.start()


def wait_all(copies):
    for copy in copies:
        copy.wait()


def project_kernel(
    x_hbm, cot_hbm, ids_hbm, wv_hbm, wg_hbm, out_hbm,
    x_ref, cot_ref, ids_ref, wv_ref, wg_ref, out_ref, sems,
):
    groups = out_ref.shape[0]
    width = 2 * LANES
    steps = x_ref.shape[1] // width
    copy = pltpu.make_async_copy
    shared = [
        copy(wv_hbm, wv_ref, sems.at[0]),
        copy(wg_hbm, wg_ref, sems.at[1]),
        copy(ids_hbm, ids_ref, sems.at[2]),
    ]
    ins, outs = [], []
    for step in range(steps):
        cols = pl.ds(step * width, width)
        ins.append(
            (
                copy(x_hbm.at[:, cols], x_ref.at[:, cols], sems.at[3 + step]),
                copy(cot_hbm.at[:, cols], cot_ref.at[:, cols], sems.at[3 + steps + step]),
            )
        )
        pair = pl.ds(2 * step, 2)
        outs.append(copy(out_ref.at[:, pair], out_hbm.at[:, pair], sems.at[3 + 2 * steps + step]))
    start_all(shared)
    for both in ins:
        start_all(both)
    wait_all(shared)
    for step in range(steps):
        wait_all(ins[step])
        cols = slice(step * width, (step + 1) * width)
        tokens = x_ref[:, cols]
        value = mm(wv_ref[...], tokens)
        gate = mm(wg_ref[...], tokens).astype(bf16).astype(f32)
        keep = jnp.where(ids_ref[:, cols] != UNKNOWN_BASE, 1.0, 0.0)
        signal = gate * (cot_ref[:, cols].astype(f32) * keep)
        for side in range(2):
            lanes = slice(side * LANES, (side + 1) * LANES)
            both = jnp.concatenate(
                [
                    value[:, lanes].reshape(groups, 8, LANES),
                    signal[:, lanes].reshape(groups, 8, LANES),
                ],
                axis=1,
            )
            out_ref[:, 2 * step + side] = both.astype(bf16)
        outs[step].start()
    wait_all(outs)


def forward(two, fwd_rows, fwd_lanes, cos_t, sin_t):
    first = mm(fwd_rows[...], two)
    outs = []
    for side in range(2):
        re = first[:BLOCKS, side * LANES : (side + 1) * LANES]
        im = first[BLOCKS:, side * LANES : (side + 1) * LANES]
        cos_v, sin_v = cos_t[...], sin_t[...]
        turned = jnp.concatenate(
            [
                (re * cos_v + im * sin_v).astype(bf16),
                (im * cos_v - re * sin_v).astype(bf16),
            ],
            axis=1,
        )
        outs.append(mm(turned, fwd_lanes[...]))
    return outs


def inverse(pair, inv_lanes, inv_rows, cos_t, sin_t):
    res, ims = [], []
    for spectrum in pair:
        mid = mm(spectrum, inv_lanes[...])
        re, im = mid[:, :LANES], mid[:, LANES:]
        cos_v, sin_v = cos_t[...], sin_t[...]
        res.append((re * cos_v - im * sin_v).astype(bf16))
        ims.append((im * cos_v + re * sin_v).astype(bf16))
    stacked = jnp.concatenate(
        [jnp.concatenate(res, axis=1), jnp.concatenate(ims, axis=1)], axis=0
    )
    return mm(inv_rows[...], stacked)


TABLE_SHAPES = (
    ((2 * BLOCKS, BLOCKS), bf16),
    ((2 * LANES, 2 * LANES), bf16),
    ((2 * LANES, 2 * LANES), bf16),
    ((BLOCKS, 2 * BLOCKS), bf16),
    ((BLOCKS, LANES), f32),
    ((BLOCKS, LANES), f32),
)
N_TABLES = len(TABLE_SHAPES)
CHUNKS = 4


def table_copies(hbm_refs, refs, sems):
    return [pltpu.make_async_copy(h, v, sems.at[i]) for i, (h, v) in enumerate(zip(hbm_refs, refs))]


def convolve_kernel(*refs):
    bias_ref, seq_hbm, refs = refs[0], refs[1], refs[2:]
    taps_hbm, tabs_hbm, refs = refs[:N_EX], refs[N_EX : N_EX + N_TABLES], refs[N_EX + N_TABLES :]
    out_hbm, pieces_hbm, refs = refs[0], refs[1 : 1 + N_EX], refs[1 + N_EX :]
    tabs, refs = refs[:N_TABLES], refs[N_TABLES:]
    seq_ref, wide_ref, taps_ref, taps_wide_ref, grad_ref, both_ref, out_ref = refs[:7]
    seq_sems, taps_sems, tab_sems, piece_sems, out_sems = refs[7:]
    fr_ref, fl_ref, il_ref, ir_ref, ct_ref, st_ref = tabs
    copy = pltpu.make_async_copy
    stride = seq_ref.shape[1]
    channels = stride // 2
    place = lax.axis_index("ex")
    own_blocks = BLOCKS // N_EX
    part = BLOCKS // CHUNKS
    seq_copies = [
        copy(seq_hbm.at[pl.ds(i * part, part)], seq_ref.at[pl.ds(i * part, part)], seq_sems.at[i])
        for i in range(CHUNKS)
    ]
    taps_copies = [copy(taps_hbm[k], taps_ref.at[k], taps_sems.at[k]) for k in range(N_EX)]
    tab_copies = table_copies(tabs_hbm, tabs, tab_sems)
    start_all(seq_copies)
    start_all(taps_copies)
    start_all(tab_copies)
    for i in range(CHUNKS):
        seq_copies[i].wait()
        rows = seq_ref[i * part : (i + 1) * part].astype(f32).reshape(part * stride, LANES)
        wide_ref[i * part * stride : (i + 1) * part * stride] = rows
    for k in range(N_EX):
        taps_copies[k].wait()
        base = lax.rem(place + (N_EX - k), N_EX) * (own_blocks * channels)
        for block in range(own_blocks):
            rows = pl.ds(pl.multiple_of(base + block * channels, channels), channels)
            taps_wide_ref[rows, :] = taps_ref[k, :, block * LANES : (block + 1) * LANES].astype(f32)
    wait_all(tab_copies)

    def transform(ref, row, row_stride):
        halves = [
            ref[pl.ds(row + side, BLOCKS, stride=row_stride), :].astype(bf16) for side in range(2)
        ]
        spectra = forward(jnp.concatenate(halves, axis=1), fr_ref, fl_ref, ct_ref, st_ref)
        return [(x[:, :LANES], x[:, LANES:]) for x in spectra]

    def times(one, other, turned):
        products = []
        for (ar, ai), (br, bi) in zip(one, other):
            if turned:
                re, im = ar * br + ai * bi, ar * bi - ai * br
            else:
                re, im = ar * br - ai * bi, ar * bi + ai * br
            products.append(jnp.concatenate([re.astype(bf16), im.astype(bf16)], axis=1))
        return inverse(products, il_ref, ir_ref, ct_ref, st_ref)

    def pair_step(step, total):
        chan = 2 * step
        value = transform(wide_ref, chan, stride)
        signal = transform(wide_ref, channels + chan, stride)
        grad = times(value, signal, True)
        for side in range(2):
            grad_ref[chan + side] = grad[:, side * LANES : (side + 1) * LANES].astype(bf16)
        filt = transform(taps_wide_ref, chan, channels)
        back = times(filt, signal, True)
        state = times(filt, value, False)
        for side in range(2):
            lanes = slice(side * LANES, (side + 1) * LANES)
            bias = bias_ref[chan + side]
            value_rows = pl.ds(chan + side, BLOCKS, stride=stride)
            signal_rows = pl.ds(channels + chan + side, BLOCKS, stride=stride)
            both_ref[value_rows, :] = back[:, lanes] + bias * wide_ref[signal_rows, :]
            both_ref[signal_rows, :] = state[:, lanes] + bias * wide_ref[value_rows, :]
        return total + jnp.sum((grad * grad).reshape(-1, 8, 2 * LANES), axis=0)

    total = lax.fori_loop(0, channels // 2, pair_step, jnp.zeros((8, 2 * LANES), f32))
    pieces = []
    for k in SEND_ORDER:
        base = pl.multiple_of(lax.rem(place + k, N_EX) * own_blocks, own_blocks)
        pieces.append(copy(grad_ref.at[:, pl.ds(base, own_blocks)], pieces_hbm[k], piece_sems.at[k]))
    whole = jnp.full((8, LANES), jnp.sum(total), f32)
    high = whole.astype(bf16).astype(f32)
    middle = (whole - high).astype(bf16).astype(f32)
    row = lax.broadcasted_iota(jnp.int32, (8, LANES), 0)
    terms = jnp.where(row == 0, high, jnp.where(row == 1, middle, whole - high - middle))
    terms = jnp.where(row < 3, terms, 0.0)
    dests, body = out_ref.shape[0], out_ref.shape[1] - 8
    share = dests // CHUNKS
    outs = []
    for i in range(CHUNKS):
        span = slice(i * share, (i + 1) * share)
        rows = both_ref[i * share * body : (i + 1) * share * body]
        out_ref[span, :body] = rows.reshape(share, body, LANES).astype(bf16)
        out_ref[span, body:] = jnp.broadcast_to(terms, (share, 8, LANES)).astype(bf16)
        span = pl.ds(i * share, share)
        outs.append(copy(out_ref.at[span], out_hbm.at[span], out_sems.at[i]))
        outs[i].start()
    start_all(pieces)
    wait_all(outs)
    wait_all(pieces)


def input_grad_kernel(
    recv_hbm, cot_hbm, ids_hbm, wv_hbm, wg_hbm, out_hbm,
    recv_ref, cot_ref, ids_ref, wv_ref, wg_ref, out_ref, sems,
):
    width = 2 * LANES
    steps = cot_ref.shape[1] // width
    copy = pltpu.make_async_copy
    shared = [
        copy(wv_hbm, wv_ref, sems.at[0]),
        copy(wg_hbm, wg_ref, sems.at[1]),
        copy(ids_hbm, ids_ref, sems.at[2]),
    ]
    ins, outs = [], []
    for step in range(steps):
        cols, rows = pl.ds(step * width, width), pl.ds(32 * step, 32)
        ins.append(
            (
                copy(recv_hbm.at[:, rows], recv_ref.at[:, rows], sems.at[3 + step]),
                copy(cot_hbm.at[:, cols], cot_ref.at[:, cols], sems.at[3 + steps + step]),
            )
        )
        outs.append(
            copy(out_ref.at[:, cols], out_hbm.at[:, cols], sems.at[3 + 2 * steps + step])
        )
    start_all(shared)
    for both in ins:
        start_all(both)
    wait_all(shared)
    back_v, back_g = wv_ref[...].T, wg_ref[...].T
    for step in range(steps):
        wait_all(ins[step])
        cols = slice(step * width, (step + 1) * width)
        keep = jnp.where(ids_ref[:, cols] != UNKNOWN_BASE, 1.0, 0.0)
        cot = cot_ref[:, cols].astype(f32) * keep
        grads, states = [], []
        for side in range(2):
            first = 32 * step + 16 * side
            both = recv_ref[:, first : first + 16].astype(f32)
            grads.append(both[:, :8].reshape(-1, LANES))
            states.append(both[:, 8:].reshape(-1, LANES))
        grad = jnp.concatenate(grads, axis=1).astype(bf16)
        gated = (jnp.concatenate(states, axis=1) * cot).astype(bf16)
        out_ref[:, cols] = (mm(back_v, grad) + mm(back_g, gated)).astype(bf16)
        outs[step].start()
    wait_all(outs)


def combine_kernel(factor_hbm, *refs):
    pieces_hbm, out_hbm = refs[:N_EX], refs[N_EX]
    factor_ref, piece_ref, total_ref, out_ref, sems = refs[N_EX + 1 :]
    copy = pltpu.make_async_copy
    ins = [copy(pieces_hbm[k], piece_ref.at[k], sems.at[k]) for k in range(N_EX)]
    factors = copy(factor_hbm, factor_ref, sems.at[N_EX])
    start_all(ins)
    factors.start()
    factors.wait()
    wait_all(ins)
    place = lax.axis_index("ex")
    channels, blocks = piece_ref.shape[1:3]
    total = 0.0
    for k in range(N_EX):
        factor = factor_ref[lax.rem(place + (N_EX - k), N_EX)]
        total = total + piece_ref[k].astype(f32) * factor
    total_ref[...] = total.reshape(total_ref.shape)
    for block in range(blocks):
        lanes = slice(block * LANES, (block + 1) * LANES)
        out_ref[:, lanes] = total_ref[pl.ds(block, channels, stride=blocks), :]
    last = copy(out_ref, out_hbm, sems.at[N_EX + 1])
    last.start()
    last.wait()


HBM = pl.BlockSpec(memory_space=pltpu.HBM)
SMEM = pl.BlockSpec(memory_space=pltpu.SMEM)


def call(body, outs, args, scratch, scalars=0, flops=0, limit=67043328):
    specs = [SMEM] * scalars + [HBM] * (len(args) - scalars)
    single = not isinstance(outs, (tuple, list))
    size = sum(math.prod(o.shape) * o.dtype.itemsize for o in ([outs] if single else outs))
    return pl.pallas_call(
        body,
        out_shape=outs,
        in_specs=specs,
        out_specs=HBM if single else tuple(HBM for _ in outs),
        scratch_shapes=list(scratch),
        cost_estimate=pl.CostEstimate(flops=flops, transcendentals=0, bytes_accessed=2 * size),
        compiler_params=pltpu.CompilerParams(vmem_limit_bytes=limit),
    )(*args)


def exchange(x, axis):
    return lax.all_to_all(x, axis, 0, 0, tiled=True)


def shift(x, places):
    ring = [(i, (i + places) % N_EX) for i in range(N_EX)]
    return lax.ppermute(x, "ex", ring)


def step(stream, cotangent, base_ids, clip_bound, w_value, w_gate, filter_taps, filter_bias):
    n_ctx = lax.axis_size("ctx")
    width, tokens = stream.shape[1:]
    channels = filter_taps.shape[0]
    blocks = tokens // LANES
    shape, vmem, dma = jax.ShapeDtypeStruct, pltpu.VMEM, pltpu.SemaphoreType.DMA
    tabs = tables()
    tab_scratch = [vmem(*s) for s in TABLE_SHAPES]
    steps = blocks // 2
    transform = 2 * 2 * channels * 512 * 256 * 128
    token_scratch = [
        vmem((width, tokens), bf16),
        vmem(base_ids.shape, jnp.int32),
        vmem((width, width), bf16),
        vmem((width, width), bf16),
    ]
    message = (n_ctx, blocks, 2 * channels, LANES)

    own_taps = filter_taps.astype(bf16)
    sent = call(
        project_kernel, shape(message, bf16),
        (stream[0], cotangent[0], base_ids, w_value, w_gate),
        [vmem((width, tokens), bf16), *token_scratch, vmem(message, bf16), dma((3 + 3 * steps,))],
        flops=4 * width * width * tokens,
    )
    seqs = exchange(sent, "ctx").reshape(BLOCKS, 2 * channels, LANES)
    taps = [own_taps] + [None] * (N_EX - 1)
    for k, source, places in RELAYS:
        taps[k] = shift(taps[source], places)

    by_channel = (channels, BLOCKS, LANES)
    piece = (channels, BLOCKS // N_EX, LANES)
    message_out = (n_ctx, blocks * 2 * channels + 8, LANES)
    outs, *pieces = call(
        convolve_kernel,
        (shape(message_out, bf16), *(shape(piece, bf16) for _ in range(N_EX))),
        (filter_bias, seqs, *taps, *tabs),
        [
            *tab_scratch,
            vmem((BLOCKS, 2 * channels, LANES), bf16),
            vmem((BLOCKS * 2 * channels, LANES), f32),
            vmem((N_EX, *filter_taps.shape), bf16),
            vmem((BLOCKS * channels, LANES), f32),
            vmem(by_channel, bf16),
            vmem((BLOCKS * 2 * channels, LANES), f32),
            vmem(message_out, bf16),
            dma((CHUNKS,)),
            dma((N_EX,)),
            dma((N_TABLES,)),
            dma((N_EX,)),
            dma((CHUNKS,)),
        ],
        scalars=1, flops=6 * transform,
    )
    back = exchange(outs, "ctx")
    owned = [pieces[0]] + [None] * (N_EX - 1)
    for k in SEND_ORDER[1:]:
        owned[k] = shift(pieces[k], k)
    terms = back[:, blocks * 2 * channels :].astype(f32)
    entries = float(tokens * n_ctx * width)
    rms = jnp.sqrt(jnp.sum(terms, axis=(0, 1)) / entries + NORM_EPS)
    factor = jnp.minimum(1.0, clip_bound.astype(f32) / rms)
    factors = exchange(jnp.broadcast_to(factor, (N_EX, 1, LANES)), "ex")
    input_grad = call(
        input_grad_kernel, shape((width, tokens), bf16),
        (back, cotangent[0], base_ids, w_value, w_gate),
        [vmem(message_out, bf16), *token_scratch, vmem((width, tokens), bf16), dma((3 + 3 * steps,))],
        flops=4 * width * width * tokens, limit=16 * 1024 * 1024,
    )
    filter_grad = call(
        combine_kernel, shape(filter_taps.shape, f32), (factors, *owned),
        [
            vmem((N_EX, 1, LANES), f32),
            vmem((N_EX, *piece), bf16),
            vmem((channels * piece[1], LANES), f32),
            vmem(filter_taps.shape, f32),
            dma((N_EX + 2,)),
        ],
    )
    return (input_grad[None], filter_grad)


def solution(mesh):
    in_specs = (
        P("ex", None, "ctx"),
        P("ex", None, "ctx"),
        P("ex", "ctx"),
        P("ex"),
        P(),
        P(),
        P("ctx", "ex"),
        P("ctx"),
    )
    out_specs = (P("ex", None, "ctx"), P("ctx", "ex"))
    return jax.shard_map(step, mesh=mesh, in_specs=in_specs, out_specs=out_specs, check_vma=False)
```

```python
import math

import jax
import jax.numpy as jnp
import numpy as np
from jax import lax
from jax.experimental import pallas as pl
from jax.experimental.pallas import tpu as pltpu
from jax.sharding import PartitionSpec as P


LANES = 128
BLOCKS = 256
SEQ = LANES * BLOCKS
N_EX = 8
SEND_ORDER = (0, 1, 7, 2, 6, 3, 5, 4)
RELAYS = ((1, 0, 1), (7, 0, 7), (2, 0, 2), (6, 0, 6), (3, 1, 2), (5, 7, 6), (4, 2, 2))
UNKNOWN_BASE = 4
NORM_EPS = 1e-06

f32 = jnp.float32
bf16 = jnp.bfloat16


def tables():
    row = np.arange(BLOCKS, dtype=np.float64)
    lane = np.arange(LANES, dtype=np.float64)
    first = 2.0 * np.pi * np.outer(row + 0.25, row) / BLOCKS
    fwd_rows = np.concatenate([np.cos(first), -np.sin(first)], axis=0)
    inv_rows = np.concatenate([np.cos(first.T), -np.sin(first.T)], axis=1) / SEQ
    twist = 2.0 * np.pi * np.outer(row + 0.25, lane) / SEQ
    second = 2.0 * np.pi * (np.outer(lane, lane) % LANES) / LANES
    cos2, sin2 = np.cos(second), np.sin(second)
    fwd_lanes = np.block([[cos2, -sin2], [sin2, cos2]])
    inv_lanes = np.block([[cos2, sin2], [-sin2, cos2]])
    half = lambda table: jnp.asarray(table.astype(np.float32)).astype(bf16)
    return (
        half(fwd_rows),
        half(fwd_lanes),
        half(inv_lanes),
        half(inv_rows),
        jnp.asarray(np.cos(twist).astype(np.float32)),
        jnp.asarray(np.sin(twist).astype(np.float32)),
    )


def mm(a, b):
    return jnp.dot(a, b, preferred_element_type=f32)


def start_all(copies):
    for copy in copies:
        copy.start()


def wait_all(copies):
    for copy in copies:
        copy.wait()


def project_kernel(
    x_hbm, cot_hbm, ids_hbm, wv_hbm, wg_hbm, out_hbm,
    x_ref, cot_ref, ids_ref, wv_ref, wg_ref, out_ref, sems,
):
    groups = out_ref.shape[0]
    width = 2 * LANES
    steps = x_ref.shape[1] // width
    copy = pltpu.make_async_copy
    shared = [
        copy(wv_hbm, wv_ref, sems.at[0]),
        copy(wg_hbm, wg_ref, sems.at[1]),
        copy(ids_hbm, ids_ref, sems.at[2]),
    ]
    ins, outs = [], []
    for step in range(steps):
        cols = pl.ds(step * width, width)
        ins.append(
            (
                copy(x_hbm.at[:, cols], x_ref.at[:, cols], sems.at[3 + step]),
                copy(cot_hbm.at[:, cols], cot_ref.at[:, cols], sems.at[3 + steps + step]),
            )
        )
        pair = pl.ds(2 * step, 2)
        outs.append(copy(out_ref.at[:, pair], out_hbm.at[:, pair], sems.at[3 + 2 * steps + step]))
    start_all(shared)
    for both in ins:
        start_all(both)
    wait_all(shared)
    for step in range(steps):
        wait_all(ins[step])
        cols = slice(step * width, (step + 1) * width)
        tokens = x_ref[:, cols]
        value = mm(wv_ref[...], tokens)
        gate = mm(wg_ref[...], tokens).astype(bf16).astype(f32)
        keep = jnp.where(ids_ref[:, cols] != UNKNOWN_BASE, 1.0, 0.0)
        signal = gate * (cot_ref[:, cols].astype(f32) * keep)
        for side in range(2):
            lanes = slice(side * LANES, (side + 1) * LANES)
            both = jnp.concatenate(
                [
                    value[:, lanes].reshape(groups, 8, LANES),
                    signal[:, lanes].reshape(groups, 8, LANES),
                ],
                axis=1,
            )
            out_ref[:, 2 * step + side] = both.astype(bf16)
        outs[step].start()
    wait_all(outs)


def forward(two, fwd_rows, fwd_lanes, cos_t, sin_t):
    first = mm(fwd_rows[...], two)
    outs = []
    for side in range(2):
        re = first[:BLOCKS, side * LANES : (side + 1) * LANES]
        im = first[BLOCKS:, side * LANES : (side + 1) * LANES]
        cos_v, sin_v = cos_t[...], sin_t[...]
        turned = jnp.concatenate(
            [
                (re * cos_v + im * sin_v).astype(bf16),
                (im * cos_v - re * sin_v).astype(bf16),
            ],
            axis=1,
        )
        outs.append(mm(turned, fwd_lanes[...]))
    return outs


def inverse(pair, inv_lanes, inv_rows, cos_t, sin_t):
    res, ims = [], []
    for spectrum in pair:
        mid = mm(spectrum, inv_lanes[...])
        re, im = mid[:, :LANES], mid[:, LANES:]
        cos_v, sin_v = cos_t[...], sin_t[...]
        res.append((re * cos_v - im * sin_v).astype(bf16))
        ims.append((im * cos_v + re * sin_v).astype(bf16))
    stacked = jnp.concatenate(
        [jnp.concatenate(res, axis=1), jnp.concatenate(ims, axis=1)], axis=0
    )
    return mm(inv_rows[...], stacked)


N_TABLES = 6
CHUNKS = 4


def convolve_kernel(*refs):
    bias_ref, seq_ref, refs = refs[0], refs[1], refs[2:]
    taps_refs, tabs, refs = refs[:N_EX], refs[N_EX : N_EX + N_TABLES], refs[N_EX + N_TABLES :]
    out_hbm, piece_refs, refs = refs[0], refs[1 : 1 + N_EX], refs[1 + N_EX :]
    wide_ref, taps_wide_ref, grad_ref, both_ref, out_ref, out_sems = refs
    fr_ref, fl_ref, il_ref, ir_ref, ct_ref, st_ref = tabs
    stride = seq_ref.shape[1]
    channels = stride // 2
    place = lax.axis_index("ex")
    own_blocks = BLOCKS // N_EX
    wide_ref[...] = seq_ref[...].astype(f32).reshape(wide_ref.shape)
    for k in range(N_EX):
        base = lax.rem(place + (N_EX - k), N_EX) * (own_blocks * channels)
        for block in range(own_blocks):
            rows = pl.ds(pl.multiple_of(base + block * channels, channels), channels)
            taps_wide_ref[rows, :] = taps_refs[k][:, block * LANES : (block + 1) * LANES].astype(f32)

    def transform(ref, row, row_stride):
        halves = [
            ref[pl.ds(row + side, BLOCKS, stride=row_stride), :].astype(bf16) for side in range(2)
        ]
        spectra = forward(jnp.concatenate(halves, axis=1), fr_ref, fl_ref, ct_ref, st_ref)
        return [(x[:, :LANES], x[:, LANES:]) for x in spectra]

    def times(one, other, turned):
        products = []
        for (ar, ai), (br, bi) in zip(one, other):
            if turned:
                re, im = ar * br + ai * bi, ar * bi - ai * br
            else:
                re, im = ar * br - ai * bi, ar * bi + ai * br
            products.append(jnp.concatenate([re.astype(bf16), im.astype(bf16)], axis=1))
        return inverse(products, il_ref, ir_ref, ct_ref, st_ref)

    def pair_step(step, total):
        chan = 2 * step
        value = transform(wide_ref, chan, stride)
        signal = transform(wide_ref, channels + chan, stride)
        grad = times(value, signal, True)
        for side in range(2):
            grad_ref[chan + side] = grad[:, side * LANES : (side + 1) * LANES].astype(bf16)
        filt = transform(taps_wide_ref, chan, channels)
        back = times(filt, signal, True)
        state = times(filt, value, False)
        for side in range(2):
            lanes = slice(side * LANES, (side + 1) * LANES)
            bias = bias_ref[chan + side]
            value_rows = pl.ds(chan + side, BLOCKS, stride=stride)
            signal_rows = pl.ds(channels + chan + side, BLOCKS, stride=stride)
            both_ref[value_rows, :] = back[:, lanes] + bias * wide_ref[signal_rows, :]
            both_ref[signal_rows, :] = state[:, lanes] + bias * wide_ref[value_rows, :]
        return total + jnp.sum((grad * grad).reshape(-1, 8, 2 * LANES), axis=0)

    total = lax.fori_loop(0, channels // 2, pair_step, jnp.zeros((8, 2 * LANES), f32))
    whole = jnp.full((8, LANES), jnp.sum(total), f32)
    high = whole.astype(bf16).astype(f32)
    middle = (whole - high).astype(bf16).astype(f32)
    row = lax.broadcasted_iota(jnp.int32, (8, LANES), 0)
    terms = jnp.where(row == 0, high, jnp.where(row == 1, middle, whole - high - middle))
    terms = jnp.where(row < 3, terms, 0.0)
    dests, body = out_ref.shape[0], out_ref.shape[1] - 8
    share = dests // CHUNKS
    outs = []
    for i in range(CHUNKS):
        span = slice(i * share, (i + 1) * share)
        rows = both_ref[i * share * body : (i + 1) * share * body]
        out_ref[span, :body] = rows.reshape(share, body, LANES).astype(bf16)
        out_ref[span, body:] = jnp.broadcast_to(terms, (share, 8, LANES)).astype(bf16)
        span = pl.ds(i * share, share)
        outs.append(pltpu.make_async_copy(out_ref.at[span], out_hbm.at[span], out_sems.at[i]))
        outs[i].start()
    for k in range(N_EX):
        base = pl.multiple_of(lax.rem(place + k, N_EX) * own_blocks, own_blocks)
        piece_refs[k][...] = grad_ref[:, pl.ds(base, own_blocks), :]
    wait_all(outs)


def input_grad_kernel(recv_ref, cot_ref, ids_ref, wv_ref, wg_ref, out_hbm, out_ref, sems):
    width = 2 * LANES
    outs = []
    back_v, back_g = wv_ref[...].T, wg_ref[...].T
    for step in range(cot_ref.shape[1] // width):
        cols = slice(step * width, (step + 1) * width)
        keep = jnp.where(ids_ref[:, cols] != UNKNOWN_BASE, 1.0, 0.0)
        cot = cot_ref[:, cols].astype(f32) * keep
        grads, states = [], []
        for side in range(2):
            first = 32 * step + 16 * side
            both = recv_ref[:, first : first + 16].astype(f32)
            grads.append(both[:, :8].reshape(-1, LANES))
            states.append(both[:, 8:].reshape(-1, LANES))
        grad = jnp.concatenate(grads, axis=1).astype(bf16)
        gated = (jnp.concatenate(states, axis=1) * cot).astype(bf16)
        out_ref[:, cols] = (mm(back_v, grad) + mm(back_g, gated)).astype(bf16)
        span = pl.ds(step * width, width)
        outs.append(pltpu.make_async_copy(out_ref.at[:, span], out_hbm.at[:, span], sems.at[step]))
        outs[step].start()
    wait_all(outs)


def combine_kernel(factor_ref, *refs):
    piece_refs, (out_hbm, total_ref, out_ref, sem) = refs[:N_EX], refs[N_EX:]
    place = lax.axis_index("ex")
    channels, blocks = piece_refs[0].shape[:2]
    total = 0.0
    for k in range(N_EX):
        factor = factor_ref[lax.rem(place + (N_EX - k), N_EX)]
        total = total + piece_refs[k][...].astype(f32) * factor
    total_ref[...] = total.reshape(total_ref.shape)
    for block in range(blocks):
        lanes = slice(block * LANES, (block + 1) * LANES)
        out_ref[:, lanes] = total_ref[pl.ds(block, channels, stride=blocks), :]
    last = pltpu.make_async_copy(out_ref, out_hbm, sem)
    last.start()
    last.wait()


HBM = pl.BlockSpec(memory_space=pltpu.HBM)
VMEM = pl.BlockSpec(memory_space=pltpu.VMEM)
SMEM = pl.BlockSpec(memory_space=pltpu.SMEM)
MIB = 1024 * 1024


def call(body, outs, args, scratch, scalars=0, kept=VMEM, flops=0, limit=16 * MIB):
    specs = [SMEM] * scalars + [kept] * (len(args) - scalars)
    single = not isinstance(outs, (tuple, list))
    size = sum(math.prod(o.shape) * o.dtype.itemsize for o in ([outs] if single else outs))
    return pl.pallas_call(
        body,
        out_shape=outs,
        in_specs=specs,
        out_specs=HBM if single else (HBM, *(VMEM for _ in outs[1:])),
        scratch_shapes=list(scratch),
        cost_estimate=pl.CostEstimate(flops=flops, transcendentals=0, bytes_accessed=2 * size),
        compiler_params=pltpu.CompilerParams(vmem_limit_bytes=limit),
    )(*args)


def exchange(x, axis):
    return lax.all_to_all(x, axis, 0, 0, tiled=True)


def shift(x, places):
    ring = [(i, (i + places) % N_EX) for i in range(N_EX)]
    return lax.ppermute(x, "ex", ring)


def step(stream, cotangent, base_ids, clip_bound, w_value, w_gate, filter_taps, filter_bias):
    n_ctx = lax.axis_size("ctx")
    width, tokens = stream.shape[1:]
    channels = filter_taps.shape[0]
    blocks = tokens // LANES
    shape, vmem, dma = jax.ShapeDtypeStruct, pltpu.VMEM, pltpu.SemaphoreType.DMA
    tabs = tables()
    steps = blocks // 2
    transform = 2 * 2 * channels * 512 * 256 * 128
    token_scratch = [
        vmem((width, tokens), bf16),
        vmem(base_ids.shape, jnp.int32),
        vmem((width, width), bf16),
        vmem((width, width), bf16),
    ]
    message = (n_ctx, blocks, 2 * channels, LANES)

    own_taps = filter_taps.astype(bf16)
    sent = call(
        project_kernel, shape(message, bf16),
        (stream[0], cotangent[0], base_ids, w_value, w_gate),
        [vmem((width, tokens), bf16), *token_scratch, vmem(message, bf16), dma((3 + 3 * steps,))],
        flops=4 * width * width * tokens, kept=HBM, limit=67043328,
    )
    seqs = exchange(sent, "ctx").reshape(BLOCKS, 2 * channels, LANES)
    taps = [own_taps] + [None] * (N_EX - 1)
    for k, source, places in RELAYS:
        taps[k] = shift(taps[source], places)

    by_channel = (channels, BLOCKS, LANES)
    piece = (channels, BLOCKS // N_EX, LANES)
    message_out = (n_ctx, blocks * 2 * channels + 8, LANES)
    outs, *pieces = call(
        convolve_kernel,
        (shape(message_out, bf16), *(shape(piece, bf16) for _ in range(N_EX))),
        (filter_bias, seqs, *taps, *tabs),
        [
            vmem((BLOCKS * 2 * channels, LANES), f32),
            vmem((BLOCKS * channels, LANES), f32),
            vmem(by_channel, bf16),
            vmem((BLOCKS * 2 * channels, LANES), f32),
            vmem(message_out, bf16),
            dma((CHUNKS,)),
        ],
        scalars=1, flops=6 * transform, limit=24 * MIB,
    )
    back = exchange(outs, "ctx")
    owned = [pieces[0]] + [None] * (N_EX - 1)
    for k in SEND_ORDER[1:]:
        owned[k] = shift(pieces[k], k)
    terms = back[:, blocks * 2 * channels :].astype(f32)
    entries = float(tokens * n_ctx * width)
    rms = jnp.sqrt(jnp.sum(terms, axis=(0, 1)) / entries + NORM_EPS)
    factor = jnp.minimum(1.0, clip_bound.astype(f32) / rms)
    factors = exchange(jnp.broadcast_to(factor, (N_EX, 1, LANES)), "ex")
    input_grad = call(
        input_grad_kernel, shape((width, tokens), bf16),
        (back, cotangent[0], base_ids, w_value, w_gate),
        [vmem((width, tokens), bf16), dma((steps,))], flops=4 * width * width * tokens,
    )
    filter_grad = call(
        combine_kernel, shape(filter_taps.shape, f32), (factors, *owned),
        [
            vmem((channels * piece[1], LANES), f32),
            vmem(filter_taps.shape, f32),
            dma,
        ],
    )
    return (input_grad[None], filter_grad)


def solution(mesh):
    in_specs = (
        P("ex", None, "ctx"),
        P("ex", None, "ctx"),
        P("ex", "ctx"),
        P("ex"),
        P(),
        P(),
        P("ctx", "ex"),
        P("ctx"),
    )
    out_specs = (P("ex", None, "ctx"), P("ctx", "ex"))
    return jax.shard_map(step, mesh=mesh, in_specs=in_specs, out_specs=out_specs, check_vma=False)
```

```python
import math

import jax
import jax.numpy as jnp
import numpy as np
from jax import lax
from jax.experimental import pallas as pl
from jax.experimental.pallas import tpu as pltpu
from jax.sharding import PartitionSpec as P


LANES = 128
BLOCKS = 256
SEQ = LANES * BLOCKS
N_EX = 8
SEND_ORDER = (0, 1, 7, 2, 6, 3, 5, 4)
RELAYS = ((2, 0, 2), (6, 0, 6), (1, 0, 1), (7, 0, 7), (3, 2, 1), (5, 6, 7), (4, 2, 2))
UNKNOWN_BASE = 4
NORM_EPS = 1e-06

f32 = jnp.float32
bf16 = jnp.bfloat16


def tables():
    row = np.arange(BLOCKS, dtype=np.float64)
    lane = np.arange(LANES, dtype=np.float64)
    first = 2.0 * np.pi * np.outer(row + 0.25, row) / BLOCKS
    fwd_rows = np.concatenate([np.cos(first), -np.sin(first)], axis=0)
    inv_rows = np.concatenate([np.cos(first.T), -np.sin(first.T)], axis=1) / SEQ
    twist = 2.0 * np.pi * np.outer(row + 0.25, lane) / SEQ
    second = 2.0 * np.pi * (np.outer(lane, lane) % LANES) / LANES
    cos2, sin2 = np.cos(second), np.sin(second)
    fwd_lanes = np.block([[cos2, -sin2], [sin2, cos2]])
    inv_lanes = np.block([[cos2, sin2], [-sin2, cos2]])
    half = lambda table: jnp.asarray(table.astype(np.float32)).astype(bf16)
    return (
        half(fwd_rows),
        half(fwd_lanes),
        half(inv_lanes),
        half(inv_rows),
        jnp.asarray(np.cos(twist).astype(np.float32)),
        jnp.asarray(np.sin(twist).astype(np.float32)),
    )


def mm(a, b):
    return jnp.dot(a, b, preferred_element_type=f32)


def start_all(copies):
    for copy in copies:
        copy.start()


def wait_all(copies):
    for copy in copies:
        copy.wait()


def project_kernel(
    x_hbm, cot_hbm, ids_hbm, wv_hbm, wg_hbm, out_hbm,
    x_ref, cot_ref, ids_ref, wv_ref, wg_ref, out_ref, sems,
):
    groups = out_ref.shape[0]
    width = 2 * LANES
    steps = x_ref.shape[1] // width
    copy = pltpu.make_async_copy
    shared = [
        copy(wv_hbm, wv_ref, sems.at[0]),
        copy(wg_hbm, wg_ref, sems.at[1]),
        copy(ids_hbm, ids_ref, sems.at[2]),
    ]
    ins, outs = [], []
    for step in range(steps):
        cols = pl.ds(step * width, width)
        ins.append(
            (
                copy(x_hbm.at[:, cols], x_ref.at[:, cols], sems.at[3 + step]),
                copy(cot_hbm.at[:, cols], cot_ref.at[:, cols], sems.at[3 + steps + step]),
            )
        )
        pair = pl.ds(2 * step, 2)
        outs.append(copy(out_ref.at[:, pair], out_hbm.at[:, pair], sems.at[3 + 2 * steps + step]))
    start_all(shared)
    for both in ins:
        start_all(both)
    wait_all(shared)
    for step in range(steps):
        wait_all(ins[step])
        cols = slice(step * width, (step + 1) * width)
        tokens = x_ref[:, cols]
        value = mm(wv_ref[...], tokens)
        gate = mm(wg_ref[...], tokens).astype(bf16).astype(f32)
        keep = jnp.where(ids_ref[:, cols] != UNKNOWN_BASE, 1.0, 0.0)
        signal = gate * (cot_ref[:, cols].astype(f32) * keep)
        for side in range(2):
            lanes = slice(side * LANES, (side + 1) * LANES)
            both = jnp.concatenate(
                [
                    value[:, lanes].reshape(groups, 8, LANES),
                    signal[:, lanes].reshape(groups, 8, LANES),
                ],
                axis=1,
            )
            out_ref[:, 2 * step + side] = both.astype(bf16)
        outs[step].start()
    wait_all(outs)


def forward(two, fwd_rows, fwd_lanes, cos_t, sin_t):
    first = mm(fwd_rows[...], two)
    outs = []
    for side in range(2):
        re = first[:BLOCKS, side * LANES : (side + 1) * LANES]
        im = first[BLOCKS:, side * LANES : (side + 1) * LANES]
        cos_v, sin_v = cos_t[...], sin_t[...]
        turned = jnp.concatenate(
            [
                (re * cos_v + im * sin_v).astype(bf16),
                (im * cos_v - re * sin_v).astype(bf16),
            ],
            axis=1,
        )
        outs.append(mm(turned, fwd_lanes[...]))
    return outs


def inverse(pair, inv_lanes, inv_rows, cos_t, sin_t):
    res, ims = [], []
    for spectrum in pair:
        mid = mm(spectrum, inv_lanes[...])
        re, im = mid[:, :LANES], mid[:, LANES:]
        cos_v, sin_v = cos_t[...], sin_t[...]
        res.append((re * cos_v - im * sin_v).astype(bf16))
        ims.append((im * cos_v + re * sin_v).astype(bf16))
    stacked = jnp.concatenate(
        [jnp.concatenate(res, axis=1), jnp.concatenate(ims, axis=1)], axis=0
    )
    return mm(inv_rows[...], stacked)


N_TABLES = 6
CHUNKS = 4


def convolve_kernel(*refs):
    bias_ref, seq_ref, refs = refs[0], refs[1], refs[2:]
    taps_refs, tabs, refs = refs[:N_EX], refs[N_EX : N_EX + N_TABLES], refs[N_EX + N_TABLES :]
    out_hbm, piece_refs, refs = refs[0], refs[1 : 1 + N_EX], refs[1 + N_EX :]
    value_ref, signal_ref, taps_wide_ref, grad_ref, back_ref, state_ref, out_ref, out_sems = refs
    fr_ref, fl_ref, il_ref, ir_ref, ct_ref, st_ref = tabs
    stride = seq_ref.shape[1]
    channels = stride // 2
    place = lax.axis_index("ex")
    own_blocks = BLOCKS // N_EX
    both = seq_ref[...].astype(f32)
    value_ref[...] = both[:, :channels].reshape(value_ref.shape)
    signal_ref[...] = both[:, channels:].reshape(signal_ref.shape)
    for k in range(N_EX):
        base = lax.rem(place + (N_EX - k), N_EX) * (own_blocks * channels)
        for block in range(own_blocks):
            rows = pl.ds(pl.multiple_of(base + block * channels, channels), channels)
            taps_wide_ref[rows, :] = taps_refs[k][:, block * LANES : (block + 1) * LANES].astype(f32)

    def transform(ref, chan):
        halves = [
            ref[pl.ds(chan + side, BLOCKS, stride=channels), :].astype(bf16) for side in range(2)
        ]
        spectra = forward(jnp.concatenate(halves, axis=1), fr_ref, fl_ref, ct_ref, st_ref)
        return halves, [(x[:, :LANES], x[:, LANES:]) for x in spectra]

    def times(one, other, turned):
        products = []
        for (ar, ai), (br, bi) in zip(one, other):
            if turned:
                re, im = ar * br + ai * bi, ar * bi - ai * br
            else:
                re, im = ar * br - ai * bi, ar * bi + ai * br
            products.append(jnp.concatenate([re.astype(bf16), im.astype(bf16)], axis=1))
        return inverse(products, il_ref, ir_ref, ct_ref, st_ref)

    def pair_step(step, total):
        chan = 2 * step
        value_in, value = transform(value_ref, chan)
        signal_in, signal = transform(signal_ref, chan)
        grad = times(value, signal, True)
        for side in range(2):
            grad_ref[chan + side] = grad[:, side * LANES : (side + 1) * LANES].astype(bf16)
        _, filt = transform(taps_wide_ref, chan)
        back = times(filt, signal, True)
        state = times(filt, value, False)
        for side in range(2):
            lanes = slice(side * LANES, (side + 1) * LANES)
            bias = bias_ref[chan + side]
            rows = pl.ds(chan + side, BLOCKS, stride=channels)
            back_ref[rows, :] = back[:, lanes] + bias * signal_in[side].astype(f32)
            state_ref[rows, :] = state[:, lanes] + bias * value_in[side].astype(f32)
        return total + jnp.sum((grad * grad).reshape(-1, 8, 2 * LANES), axis=0)

    total = lax.fori_loop(0, channels // 2, pair_step, jnp.zeros((8, 2 * LANES), f32))
    whole = jnp.full((8, LANES), jnp.sum(total), f32)
    high = whole.astype(bf16).astype(f32)
    middle = (whole - high).astype(bf16).astype(f32)
    row = lax.broadcasted_iota(jnp.int32, (8, LANES), 0)
    terms = jnp.where(row == 0, high, jnp.where(row == 1, middle, whole - high - middle))
    terms = jnp.where(row < 3, terms, 0.0)
    dests, body = out_ref.shape[0], out_ref.shape[1] - 8
    share = dests // CHUNKS
    outs = []
    for i in range(CHUNKS):
        span = slice(i * share, (i + 1) * share)
        rows = slice(i * share * body // 2, (i + 1) * share * body // 2)
        pair = [ref[rows].reshape(-1, channels, LANES) for ref in (back_ref, state_ref)]
        both = jnp.concatenate(pair, axis=1)
        out_ref[span, :body] = both.reshape(share, body, LANES).astype(bf16)
        out_ref[span, body:] = jnp.broadcast_to(terms, (share, 8, LANES)).astype(bf16)
        span = pl.ds(i * share, share)
        outs.append(pltpu.make_async_copy(out_ref.at[span], out_hbm.at[span], out_sems.at[i]))
        outs[i].start()
    for k in range(N_EX):
        base = pl.multiple_of(lax.rem(place + k, N_EX) * own_blocks, own_blocks)
        piece_refs[k][...] = grad_ref[:, pl.ds(base, own_blocks), :]
    wait_all(outs)


def input_grad_kernel(recv_ref, cot_ref, ids_ref, wv_ref, wg_ref, out_hbm, out_ref, sems):
    width = 2 * LANES
    outs = []
    back_v, back_g = wv_ref[...].T, wg_ref[...].T
    for step in range(cot_ref.shape[1] // width):
        cols = slice(step * width, (step + 1) * width)
        keep = jnp.where(ids_ref[:, cols] != UNKNOWN_BASE, 1.0, 0.0)
        cot = cot_ref[:, cols].astype(f32) * keep
        grads, states = [], []
        for side in range(2):
            first = 32 * step + 16 * side
            both = recv_ref[:, first : first + 16].astype(f32)
            grads.append(both[:, :8].reshape(-1, LANES))
            states.append(both[:, 8:].reshape(-1, LANES))
        grad = jnp.concatenate(grads, axis=1).astype(bf16)
        gated = (jnp.concatenate(states, axis=1) * cot).astype(bf16)
        out_ref[:, cols] = (mm(back_v, grad) + mm(back_g, gated)).astype(bf16)
        span = pl.ds(step * width, width)
        outs.append(pltpu.make_async_copy(out_ref.at[:, span], out_hbm.at[:, span], sems.at[step]))
        outs[step].start()
    wait_all(outs)


def combine_kernel(factor_ref, *refs):
    piece_refs, (out_hbm, total_ref, out_ref, sem) = refs[:N_EX], refs[N_EX:]
    place = lax.axis_index("ex")
    channels, blocks = piece_refs[0].shape[:2]
    total = 0.0
    for k in range(N_EX):
        factor = factor_ref[lax.rem(place + (N_EX - k), N_EX)]
        total = total + piece_refs[k][...].astype(f32) * factor
    total_ref[...] = total.reshape(total_ref.shape)
    for block in range(blocks):
        lanes = slice(block * LANES, (block + 1) * LANES)
        out_ref[:, lanes] = total_ref[pl.ds(block, channels, stride=blocks), :]
    last = pltpu.make_async_copy(out_ref, out_hbm, sem)
    last.start()
    last.wait()


HBM = pl.BlockSpec(memory_space=pltpu.HBM)
VMEM = pl.BlockSpec(memory_space=pltpu.VMEM)
SMEM = pl.BlockSpec(memory_space=pltpu.SMEM)
MIB = 1024 * 1024


def call(body, outs, args, scratch, scalars=0, kept=VMEM, flops=0, limit=16 * MIB):
    specs = [SMEM] * scalars + [kept] * (len(args) - scalars)
    single = not isinstance(outs, (tuple, list))
    size = sum(math.prod(o.shape) * o.dtype.itemsize for o in ([outs] if single else outs))
    return pl.pallas_call(
        body,
        out_shape=outs,
        in_specs=specs,
        out_specs=HBM if single else (HBM, *(VMEM for _ in outs[1:])),
        scratch_shapes=list(scratch),
        cost_estimate=pl.CostEstimate(flops=flops, transcendentals=0, bytes_accessed=2 * size),
        compiler_params=pltpu.CompilerParams(vmem_limit_bytes=limit),
    )(*args)


def exchange(x, axis):
    return lax.all_to_all(x, axis, 0, 0, tiled=True)


def shift(x, places):
    ring = [(i, (i + places) % N_EX) for i in range(N_EX)]
    return lax.ppermute(x, "ex", ring)


def step(stream, cotangent, base_ids, clip_bound, w_value, w_gate, filter_taps, filter_bias):
    n_ctx = lax.axis_size("ctx")
    width, tokens = stream.shape[1:]
    channels = filter_taps.shape[0]
    blocks = tokens // LANES
    shape, vmem, dma = jax.ShapeDtypeStruct, pltpu.VMEM, pltpu.SemaphoreType.DMA
    tabs = tables()
    steps = blocks // 2
    transform = 2 * 2 * channels * 512 * 256 * 128
    token_scratch = [
        vmem((width, tokens), bf16),
        vmem(base_ids.shape, jnp.int32),
        vmem((width, width), bf16),
        vmem((width, width), bf16),
    ]
    message = (n_ctx, blocks, 2 * channels, LANES)

    own_taps = filter_taps.astype(bf16)
    sent = call(
        project_kernel, shape(message, bf16),
        (stream[0], cotangent[0], base_ids, w_value, w_gate),
        [vmem((width, tokens), bf16), *token_scratch, vmem(message, bf16), dma((3 + 3 * steps,))],
        flops=4 * width * width * tokens, kept=HBM, limit=67043328,
    )
    seqs = exchange(sent, "ctx").reshape(BLOCKS, 2 * channels, LANES)
    taps = [own_taps] + [None] * (N_EX - 1)
    for k, source, places in RELAYS:
        taps[k] = shift(taps[source], places)

    by_channel = (channels, BLOCKS, LANES)
    piece = (channels, BLOCKS // N_EX, LANES)
    message_out = (n_ctx, blocks * 2 * channels + 8, LANES)
    outs, *pieces = call(
        convolve_kernel,
        (shape(message_out, bf16), *(shape(piece, bf16) for _ in range(N_EX))),
        (filter_bias, seqs, *taps, *tabs),
        [
            *(vmem((BLOCKS * channels, LANES), f32) for _ in range(3)),
            vmem(by_channel, bf16),
            *(vmem((BLOCKS * channels, LANES), f32) for _ in range(2)),
            vmem(message_out, bf16),
            dma((CHUNKS,)),
        ],
        scalars=1, flops=6 * transform, limit=24 * MIB,
    )
    back = exchange(outs, "ctx")
    owned = [pieces[0]] + [None] * (N_EX - 1)
    for k in SEND_ORDER[1:]:
        owned[k] = shift(pieces[k], k)
    terms = back[:, blocks * 2 * channels :].astype(f32)
    entries = float(tokens * n_ctx * width)
    rms = jnp.sqrt(jnp.sum(terms, axis=(0, 1)) / entries + NORM_EPS)
    factor = jnp.minimum(1.0, clip_bound.astype(f32) / rms)
    factors = exchange(jnp.broadcast_to(factor, (N_EX, 1, LANES)), "ex")
    input_grad = call(
        input_grad_kernel, shape((width, tokens), bf16),
        (back, cotangent[0], base_ids, w_value, w_gate),
        [vmem((width, tokens), bf16), dma((steps,))], flops=4 * width * width * tokens,
    )
    filter_grad = call(
        combine_kernel, shape(filter_taps.shape, f32), (factors, *owned),
        [
            vmem((channels * piece[1], LANES), f32),
            vmem(filter_taps.shape, f32),
            dma,
        ],
    )
    return (input_grad[None], filter_grad)


def solution(mesh):
    in_specs = (
        P("ex", None, "ctx"),
        P("ex", None, "ctx"),
        P("ex", "ctx"),
        P("ex"),
        P(),
        P(),
        P("ctx", "ex"),
        P("ctx"),
    )
    out_specs = (P("ex", None, "ctx"), P("ctx", "ex"))
    return jax.shard_map(step, mesh=mesh, in_specs=in_specs, out_specs=out_specs, check_vma=False)
```

```python
import math

import jax
import jax.numpy as jnp
import numpy as np
from jax import lax
from jax.experimental import pallas as pl
from jax.experimental.pallas import tpu as pltpu
from jax.sharding import PartitionSpec as P


LANES = 128
BLOCKS = 256
SEQ = LANES * BLOCKS
N_EX = 8
SEND_ORDER = (0, 1, 7, 2, 6, 3, 5, 4)
RELAYS = ((2, 0, 2), (6, 0, 6), (1, 0, 1), (7, 0, 7), (3, 2, 1), (5, 6, 7), (4, 2, 2))
PROJECT = 4
UNKNOWN_BASE = 4
NORM_EPS = 1e-06

f32 = jnp.float32
bf16 = jnp.bfloat16


def tables():
    row = np.arange(BLOCKS, dtype=np.float64)
    lane = np.arange(LANES, dtype=np.float64)
    first = 2.0 * np.pi * np.outer(row + 0.25, row) / BLOCKS
    fwd_rows = np.concatenate([np.cos(first), -np.sin(first)], axis=0)
    inv_rows = np.concatenate([np.cos(first.T), -np.sin(first.T)], axis=1) / SEQ
    twist = 2.0 * np.pi * np.outer(row + 0.25, lane) / SEQ
    second = 2.0 * np.pi * (np.outer(lane, lane) % LANES) / LANES
    cos2, sin2 = np.cos(second), np.sin(second)
    fwd_lanes = np.block([[cos2, -sin2], [sin2, cos2]])
    inv_lanes = np.block([[cos2, sin2], [-sin2, cos2]])
    half = lambda table: jnp.asarray(table.astype(np.float32)).astype(bf16)
    return (
        half(fwd_rows),
        half(fwd_lanes),
        half(inv_lanes),
        half(inv_rows),
        jnp.asarray(np.cos(twist).astype(np.float32)),
        jnp.asarray(np.sin(twist).astype(np.float32)),
    )


def mm(a, b):
    return jnp.dot(a, b, preferred_element_type=f32)


def start_all(copies):
    for copy in copies:
        copy.start()


def wait_all(copies):
    for copy in copies:
        copy.wait()


def project_kernel(
    x_hbm, cot_hbm, ids_hbm, wv_hbm, wg_hbm, out_hbm,
    x_ref, cot_ref, ids_ref, wv_ref, wg_ref, out_ref, sems,
):
    groups = out_ref.shape[0]
    width = PROJECT * LANES
    steps = x_ref.shape[1] // width
    copy = pltpu.make_async_copy
    shared = [
        copy(wv_hbm, wv_ref, sems.at[0]),
        copy(wg_hbm, wg_ref, sems.at[1]),
        copy(ids_hbm, ids_ref, sems.at[2]),
    ]
    ins, outs = [], []
    for step in range(steps):
        cols = pl.ds(step * width, width)
        ins.append(
            (
                copy(x_hbm.at[:, cols], x_ref.at[:, cols], sems.at[3 + step]),
                copy(cot_hbm.at[:, cols], cot_ref.at[:, cols], sems.at[3 + steps + step]),
            )
        )
        pair = pl.ds(PROJECT * step, PROJECT)
        outs.append(copy(out_ref.at[:, pair], out_hbm.at[:, pair], sems.at[3 + 2 * steps + step]))
    start_all(shared)
    for both in ins:
        start_all(both)
    wait_all(shared)
    for step in range(steps):
        wait_all(ins[step])
        cols = slice(step * width, (step + 1) * width)
        tokens = x_ref[:, cols]
        value = mm(wv_ref[...], tokens)
        gate = mm(wg_ref[...], tokens).astype(bf16).astype(f32)
        keep = jnp.where(ids_ref[:, cols] != UNKNOWN_BASE, 1.0, 0.0)
        signal = gate * (cot_ref[:, cols].astype(f32) * keep)
        for side in range(PROJECT):
            lanes = slice(side * LANES, (side + 1) * LANES)
            both = jnp.concatenate(
                [
                    value[:, lanes].reshape(groups, 8, LANES),
                    signal[:, lanes].reshape(groups, 8, LANES),
                ],
                axis=1,
            )
            out_ref[:, PROJECT * step + side] = both.astype(bf16)
        outs[step].start()
    wait_all(outs)


def forward(two, fwd_rows, fwd_lanes, cos_t, sin_t):
    first = mm(fwd_rows[...], two)
    outs = []
    for side in range(2):
        re = first[:BLOCKS, side * LANES : (side + 1) * LANES]
        im = first[BLOCKS:, side * LANES : (side + 1) * LANES]
        cos_v, sin_v = cos_t[...], sin_t[...]
        turned = jnp.concatenate(
            [
                (re * cos_v + im * sin_v).astype(bf16),
                (im * cos_v - re * sin_v).astype(bf16),
            ],
            axis=1,
        )
        outs.append(mm(turned, fwd_lanes[...]))
    return outs


def inverse(pair, inv_lanes, inv_rows, cos_t, sin_t):
    res, ims = [], []
    for spectrum in pair:
        mid = mm(spectrum, inv_lanes[...])
        re, im = mid[:, :LANES], mid[:, LANES:]
        cos_v, sin_v = cos_t[...], sin_t[...]
        res.append((re * cos_v - im * sin_v).astype(bf16))
        ims.append((im * cos_v + re * sin_v).astype(bf16))
    stacked = jnp.concatenate(
        [jnp.concatenate(res, axis=1), jnp.concatenate(ims, axis=1)], axis=0
    )
    return mm(inv_rows[...], stacked)


N_TABLES = 6
CHUNKS = 4


def convolve_kernel(*refs):
    bias_ref, seq_ref, refs = refs[0], refs[1], refs[2:]
    taps_refs, tabs, refs = refs[:N_EX], refs[N_EX : N_EX + N_TABLES], refs[N_EX + N_TABLES :]
    out_hbm, piece_refs, refs = refs[0], refs[1 : 1 + N_EX], refs[1 + N_EX :]
    value_ref, signal_ref, taps_wide_ref, grad_ref, back_ref, state_ref, out_ref, out_sems = refs
    fr_ref, fl_ref, il_ref, ir_ref, ct_ref, st_ref = tabs
    stride = seq_ref.shape[1]
    channels = stride // 2
    place = lax.axis_index("ex")
    own_blocks = BLOCKS // N_EX
    both = seq_ref[...].astype(f32)
    value_ref[...] = both[:, :channels].reshape(value_ref.shape)
    signal_ref[...] = both[:, channels:].reshape(signal_ref.shape)
    for k in range(N_EX):
        base = lax.rem(place + (N_EX - k), N_EX) * (own_blocks * channels)
        for block in range(own_blocks):
            rows = pl.ds(pl.multiple_of(base + block * channels, channels), channels)
            taps_wide_ref[rows, :] = taps_refs[k][:, block * LANES : (block + 1) * LANES].astype(f32)

    def transform(ref, chan):
        halves = [
            ref[pl.ds(chan + side, BLOCKS, stride=channels), :].astype(bf16) for side in range(2)
        ]
        spectra = forward(jnp.concatenate(halves, axis=1), fr_ref, fl_ref, ct_ref, st_ref)
        return halves, [(x[:, :LANES], x[:, LANES:]) for x in spectra]

    def times(one, other, turned):
        products = []
        for (ar, ai), (br, bi) in zip(one, other):
            if turned:
                re, im = ar * br + ai * bi, ar * bi - ai * br
            else:
                re, im = ar * br - ai * bi, ar * bi + ai * br
            products.append(jnp.concatenate([re.astype(bf16), im.astype(bf16)], axis=1))
        return inverse(products, il_ref, ir_ref, ct_ref, st_ref)

    def pair_step(step, total):
        chan = 2 * step
        value_in, value = transform(value_ref, chan)
        signal_in, signal = transform(signal_ref, chan)
        _, filt = transform(taps_wide_ref, chan)
        state = times(filt, value, False)
        back = times(filt, signal, True)
        grad = times(value, signal, True)
        for side in range(2):
            grad_ref[chan + side] = grad[:, side * LANES : (side + 1) * LANES].astype(bf16)
        for side in range(2):
            lanes = slice(side * LANES, (side + 1) * LANES)
            bias = bias_ref[chan + side]
            rows = pl.ds(chan + side, BLOCKS, stride=channels)
            back_ref[rows, :] = back[:, lanes] + bias * signal_in[side].astype(f32)
            state_ref[rows, :] = state[:, lanes] + bias * value_in[side].astype(f32)
        return total + jnp.sum((grad * grad).reshape(-1, 8, 2 * LANES), axis=0)

    total = lax.fori_loop(0, channels // 2, pair_step, jnp.zeros((8, 2 * LANES), f32))
    whole = jnp.full((8, LANES), jnp.sum(total), f32)
    high = whole.astype(bf16).astype(f32)
    middle = (whole - high).astype(bf16).astype(f32)
    row = lax.broadcasted_iota(jnp.int32, (8, LANES), 0)
    terms = jnp.where(row == 0, high, jnp.where(row == 1, middle, whole - high - middle))
    terms = jnp.where(row < 3, terms, 0.0)
    dests, body = out_ref.shape[0], out_ref.shape[1] - 8
    share = dests // CHUNKS
    outs = []
    for i in range(CHUNKS):
        span = slice(i * share, (i + 1) * share)
        rows = slice(i * share * body // 2, (i + 1) * share * body // 2)
        pair = [ref[rows].reshape(-1, channels, LANES) for ref in (back_ref, state_ref)]
        both = jnp.concatenate(pair, axis=1)
        out_ref[span, :body] = both.reshape(share, body, LANES).astype(bf16)
        out_ref[span, body:] = jnp.broadcast_to(terms, (share, 8, LANES)).astype(bf16)
        span = pl.ds(i * share, share)
        outs.append(pltpu.make_async_copy(out_ref.at[span], out_hbm.at[span], out_sems.at[i]))
        outs[i].start()
    for k in range(N_EX):
        base = pl.multiple_of(lax.rem(place + k, N_EX) * own_blocks, own_blocks)
        piece_refs[k][...] = grad_ref[:, pl.ds(base, own_blocks), :]
    wait_all(outs)


def input_grad_kernel(recv_ref, cot_ref, ids_ref, wv_ref, wg_ref, out_hbm, out_ref, sems):
    width = 2 * LANES
    outs = []
    back_v, back_g = wv_ref[...].T, wg_ref[...].T
    for step in range(cot_ref.shape[1] // width):
        cols = slice(step * width, (step + 1) * width)
        keep = jnp.where(ids_ref[:, cols] != UNKNOWN_BASE, 1.0, 0.0)
        cot = cot_ref[:, cols].astype(f32) * keep
        grads, states = [], []
        for side in range(2):
            first = 32 * step + 16 * side
            both = recv_ref[:, first : first + 16].astype(f32)
            grads.append(both[:, :8].reshape(-1, LANES))
            states.append(both[:, 8:].reshape(-1, LANES))
        grad = jnp.concatenate(grads, axis=1).astype(bf16)
        gated = (jnp.concatenate(states, axis=1) * cot).astype(bf16)
        out_ref[:, cols] = (mm(back_v, grad) + mm(back_g, gated)).astype(bf16)
        span = pl.ds(step * width, width)
        outs.append(pltpu.make_async_copy(out_ref.at[:, span], out_hbm.at[:, span], sems.at[step]))
        outs[step].start()
    wait_all(outs)


def combine_kernel(factor_ref, *refs):
    piece_refs, (out_hbm, total_ref, out_ref, sem) = refs[:N_EX], refs[N_EX:]
    place = lax.axis_index("ex")
    channels, blocks = piece_refs[0].shape[:2]
    total = 0.0
    for k in range(N_EX):
        factor = factor_ref[lax.rem(place + (N_EX - k), N_EX)]
        total = total + piece_refs[k][...].astype(f32) * factor
    total_ref[...] = total.reshape(total_ref.shape)
    for block in range(blocks):
        lanes = slice(block * LANES, (block + 1) * LANES)
        out_ref[:, lanes] = total_ref[pl.ds(block, channels, stride=blocks), :]
    last = pltpu.make_async_copy(out_ref, out_hbm, sem)
    last.start()
    last.wait()


HBM = pl.BlockSpec(memory_space=pltpu.HBM)
VMEM = pl.BlockSpec(memory_space=pltpu.VMEM)
SMEM = pl.BlockSpec(memory_space=pltpu.SMEM)
MIB = 1024 * 1024


def call(body, outs, args, scratch, scalars=0, kept=VMEM, flops=0, limit=16 * MIB):
    specs = [SMEM] * scalars + [kept] * (len(args) - scalars)
    single = not isinstance(outs, (tuple, list))
    size = sum(math.prod(o.shape) * o.dtype.itemsize for o in ([outs] if single else outs))
    return pl.pallas_call(
        body,
        out_shape=outs,
        in_specs=specs,
        out_specs=HBM if single else (HBM, *(VMEM for _ in outs[1:])),
        scratch_shapes=list(scratch),
        cost_estimate=pl.CostEstimate(flops=flops, transcendentals=0, bytes_accessed=2 * size),
        compiler_params=pltpu.CompilerParams(vmem_limit_bytes=limit),
    )(*args)


def exchange(x, axis):
    return lax.all_to_all(x, axis, 0, 0, tiled=True)


def shift(x, places):
    ring = [(i, (i + places) % N_EX) for i in range(N_EX)]
    return lax.ppermute(x, "ex", ring)


def step(stream, cotangent, base_ids, clip_bound, w_value, w_gate, filter_taps, filter_bias):
    n_ctx = lax.axis_size("ctx")
    width, tokens = stream.shape[1:]
    channels = filter_taps.shape[0]
    blocks = tokens // LANES
    shape, vmem, dma = jax.ShapeDtypeStruct, pltpu.VMEM, pltpu.SemaphoreType.DMA
    tabs = tables()
    steps = blocks // 2
    transform = 2 * 2 * channels * 512 * 256 * 128
    token_scratch = [
        vmem((width, tokens), bf16),
        vmem(base_ids.shape, jnp.int32),
        vmem((width, width), bf16),
        vmem((width, width), bf16),
    ]
    message = (n_ctx, blocks, 2 * channels, LANES)

    own_taps = filter_taps.astype(bf16)
    sent = call(
        project_kernel, shape(message, bf16),
        (stream[0], cotangent[0], base_ids, w_value, w_gate),
        [vmem((width, tokens), bf16), *token_scratch, vmem(message, bf16), dma((3 + 3 * blocks // PROJECT,))],
        flops=4 * width * width * tokens, kept=HBM, limit=67043328,
    )
    seqs = exchange(sent, "ctx").reshape(BLOCKS, 2 * channels, LANES)
    taps = [own_taps] + [None] * (N_EX - 1)
    for k, source, places in RELAYS:
        taps[k] = shift(taps[source], places)

    by_channel = (channels, BLOCKS, LANES)
    piece = (channels, BLOCKS // N_EX, LANES)
    message_out = (n_ctx, blocks * 2 * channels + 8, LANES)
    outs, *pieces = call(
        convolve_kernel,
        (shape(message_out, bf16), *(shape(piece, bf16) for _ in range(N_EX))),
        (filter_bias, seqs, *taps, *tabs),
        [
            *(vmem((BLOCKS * channels, LANES), f32) for _ in range(3)),
            vmem(by_channel, bf16),
            *(vmem((BLOCKS * channels, LANES), f32) for _ in range(2)),
            vmem(message_out, bf16),
            dma((CHUNKS,)),
        ],
        scalars=1, flops=6 * transform, limit=24 * MIB,
    )
    back = exchange(outs, "ctx")
    owned = [pieces[0]] + [None] * (N_EX - 1)
    for k in SEND_ORDER[1:]:
        owned[k] = shift(pieces[k], k)
    terms = back[:, blocks * 2 * channels :].astype(f32)
    entries = float(tokens * n_ctx * width)
    rms = jnp.sqrt(jnp.sum(terms, axis=(0, 1)) / entries + NORM_EPS)
    factor = jnp.minimum(1.0, clip_bound.astype(f32) / rms)
    factors = exchange(jnp.broadcast_to(factor, (N_EX, 1, LANES)), "ex")
    input_grad = call(
        input_grad_kernel, shape((width, tokens), bf16),
        (back, cotangent[0], base_ids, w_value, w_gate),
        [vmem((width, tokens), bf16), dma((steps,))], flops=4 * width * width * tokens,
    )
    filter_grad = call(
        combine_kernel, shape(filter_taps.shape, f32), (factors, *owned),
        [
            vmem((channels * piece[1], LANES), f32),
            vmem(filter_taps.shape, f32),
            dma,
        ],
    )
    return (input_grad[None], filter_grad)


def solution(mesh):
    in_specs = (
        P("ex", None, "ctx"),
        P("ex", None, "ctx"),
        P("ex", "ctx"),
        P("ex"),
        P(),
        P(),
        P("ctx", "ex"),
        P("ctx"),
    )
    out_specs = (P("ex", None, "ctx"), P("ctx", "ex"))
    return jax.shard_map(step, mesh=mesh, in_specs=in_specs, out_specs=out_specs, check_vma=False)
```
